128 devices in a mesh: cls: 128 (over y, x, z, core).
Axes of the slice: x: 4, y: 4, z: 4, core: 2. Of those that a mesh axis runs over, the one named last changes fastest.
Arguments:
- features: bfloat16 [2048, 12544], P('cls'), may hold values from -6 to 6
- fc_weight: bfloat16 [12544, 512], replicated, may hold values from -0.0546875 to 0.0546875
- centers: bfloat16 [524288, 512], P('cls'), may hold values from -6 to 6
- labels: int32 [2048], replicated, may hold values from 0 to 524287
Outputs:
- loss: float32 [2048], P('cls')
- grad_centers: bfloat16 [524288, 512], P('cls')
- grad_fc: float32 [12544, 512], P('cls')
The draws below stay inside these ranges and needn't reach their ends.
All inputs are finite; a program needn't handle non-finite values.
Results may differ from the reference program's by a relative error of at most 0.0078.
Values may be sent and summed in bfloat16 or wider, within the bound.
A program may use at most 128 MiB of HBM per device.

```python
import math
import jax
import jax.numpy as jnp
from jax import lax

D = 512
F = 12544
C_DEV = 4096
B = 2048
C = 524288
N_CLS = 128


def place_ends(entries, own_key, least, top_value):
    longest = entries.shape.index(max(entries.shape))
    spots = []
    for shift in (0, 1):
        where = [jax.random.randint(jax.random.fold_in(own_key, axis), (), 0, length) for axis, length in enumerate(entries.shape)]
        where[longest] = (where[longest] + shift) % entries.shape[longest]
        spots.append(tuple(where))
    return entries.at[spots[0]].set(least).at[spots[1]].set(top_value)


def levels(key, shape, cuts, smallest, largest):
    level, own = 1.0, jax.random.fold_in(key, 6)
    for position, blocks in cuts:
        steps = jnp.exp(jax.random.uniform(jax.random.fold_in(own, position), (blocks,), jnp.float32, smallest / len(cuts), largest / len(cuts)))
        level = level * jnp.repeat(steps, shape[position] // blocks).reshape([-1 if axis == position else 1 for axis in range(len(shape))])
    return level


def gaussian(key, shape, deviation, reach, split=(), held_as=jnp.bfloat16):
    result = deviation * jax.random.normal(key, shape, jnp.float32)
    if split:
        result = result * levels(key, shape, split, -0.22, 0.18)
    return jnp.clip(result, -reach, reach).astype(held_as)


def setup_inputs(seed: int = 0) -> dict:
    key_list = jax.random.split(jax.random.key(seed), 5)
    return {
        "features": gaussian(key_list[0], (B, F), 1.0, 6.0, ((0, 128),)),
        "fc_weight": gaussian(key_list[1], (F, D), F ** -0.5, 0.0546875),
        "centers": gaussian(key_list[2], (C, D), 1.0, 6.0, ((0, 128),)),
        "labels": place_ends(jax.random.randint(key_list[3], (B,), 0, C), jax.random.fold_in(key_list[3], 1), 0, C - 1).astype(jnp.int32),
    }


logit_scale = 64.0
cos_margin = math.cos(0.5)
sin_margin = math.sin(0.5)
epsilon = 1e-06

def inverse_norm(values):
    return lax.rsqrt(lax.optimization_barrier(jnp.sum(values * values, axis=1, keepdims=True)) + epsilon)

def margin_logits(emb_low, center_low, labels, offset):
    cosines = jnp.dot(emb_low, center_low.T, preferred_element_type=jnp.float32)
    local_ids = labels - offset
    is_target = local_ids[:, None] == lax.broadcasted_iota(jnp.int32, (1, center_low.shape[0]), 1)
    target_cos = lax.optimization_barrier(jnp.sum(jnp.where(is_target, cosines, 0.0), axis=1))
    target_sine = jnp.sqrt(1.0 - target_cos * target_cos)
    margined = target_cos * cos_margin - target_sine * sin_margin
    logits = logit_scale * jnp.where(is_target, margined[:, None], cosines)
    slope = cos_margin + sin_margin * target_cos / target_sine
    return (logits, is_target, slope)

def center_parts(block):
    center_float = block.astype(jnp.float32)
    inv_center = inverse_norm(center_float)
    center_dir = center_float * inv_center
    return (inv_center, center_dir, center_dir.astype(jnp.bfloat16))

def reference(features, fc_weight, centers, labels):
    batch = labels.shape[0]
    embedded = jnp.dot(features, fc_weight, preferred_element_type=jnp.float32).astype(jnp.bfloat16)
    emb_float = embedded.astype(jnp.float32)
    inv_emb = inverse_norm(emb_float)
    emb_dir = emb_float * inv_emb
    emb_low = emb_dir.astype(jnp.bfloat16)
    blocks = centers.reshape(N_CLS, C_DEV, D)
    shard_ids = jnp.arange(N_CLS, dtype=jnp.int32)

    def stats_step(carry, item):
        shard, block = item
        unused_inv, unused_dir, center_low = center_parts(block)
        logits, is_target, unused_slope = margin_logits(emb_low, center_low, labels, shard * C_DEV)
        running_sum, target_sum = carry
        running_sum = running_sum + lax.optimization_barrier(jnp.sum(jnp.exp(logits - logit_scale), axis=1))
        target_sum = target_sum + lax.optimization_barrier(jnp.sum(jnp.where(is_target, logits, 0.0), axis=1))
        return ((running_sum, target_sum), None)
    start_stats = (jnp.zeros((batch,), jnp.float32), jnp.zeros((batch,), jnp.float32))
    (row_sum, target_sum), unused_out = lax.scan(stats_step, start_stats, (shard_ids, blocks))
    log_total = logit_scale + jnp.log(row_sum)
    loss = log_total - target_sum

    def grad_step(grad_dir, item):
        shard, block = item
        inv_center, center_dir, center_low = center_parts(block)
        logits, is_target, slope = margin_logits(emb_low, center_low, labels, shard * C_DEV)
        probs = jnp.exp(logits - log_total[:, None])
        grad_cos = (logit_scale * (probs - is_target.astype(jnp.float32)) * jnp.where(is_target, slope[:, None], 1.0)).astype(jnp.bfloat16)
        grad_unit = jnp.dot(grad_cos.T, emb_low, preferred_element_type=jnp.float32)
        grad_center = ((grad_unit - center_dir * lax.optimization_barrier(jnp.sum(grad_unit * center_dir, axis=1, keepdims=True))) * inv_center).astype(jnp.bfloat16)
        grad_dir = grad_dir + jnp.dot(grad_cos, center_low, preferred_element_type=jnp.float32)
        return (grad_dir, grad_center)
    grad_dir, grad_blocks = lax.scan(grad_step, jnp.zeros((batch, D), jnp.float32), (shard_ids, blocks))
    grad_centers = grad_blocks.reshape(N_CLS * C_DEV, D)
    grad_emb = ((grad_dir - emb_dir * lax.optimization_barrier(jnp.sum(grad_dir * emb_dir, axis=1, keepdims=True))) * inv_emb).astype(jnp.bfloat16)
    grad_fc = jnp.dot(features.T, grad_emb, preferred_element_type=jnp.float32)
    return (loss, grad_centers, grad_fc)
```

```python
import functools
import math

import jax
import jax.numpy as jnp
from jax import lax
from jax.experimental import pallas as pl
from jax.experimental.pallas import tpu as pltpu
from jax.sharding import Mesh
from jax.sharding import PartitionSpec as P

CLS = ("cls_0", "cls_1", "cls_2", "cls_3")
MESH = pl.DeviceIdType.MESH

logit_scale = 64.0
cos_margin = math.cos(0.5)
sin_margin = math.sin(0.5)
epsilon = 1e-06
exp2_scale = logit_scale / math.log(2.0)

N = 128
D = 512
F = 12544
F_DEV = F // N
OWN = 16
CLASSES = 4096
BT = 512
W_CHUNK = 1792
N_W = F // W_CHUNK
JA = 1024
JB = 1024
JC = 512

ORDERS = ((0, 1, 2), (1, 2, 0), (2, 0, 1), (0, 2, 1))

f32 = jnp.float32
bf16 = jnp.bfloat16


def last_dims(a, b):
    return lax.dot_general(a, b, (((1,), (1,)), ((), ())), preferred_element_type=f32)


def plain_dot(a, b):
    return lax.dot_general(a, b, (((1,), (0,)), ((), ())), preferred_element_type=f32)


def eye(n):
    r = lax.broadcasted_iota(jnp.int32, (n, n), 0)
    c = lax.broadcasted_iota(jnp.int32, (n, n), 1)
    return (r == c).astype(f32).astype(bf16)


def kernel(
    feat, w_hbm, centers_hbm, labels,
    loss_out, fc_out, gc_hbm,
    E, cen, clow, ct, tt, emb, gemb, gt, G, rb0, gs, rb1, gs2, rb2, gs3, rb3, cols,
    own_emb, ar_send, ar_recv, rows,
    w_sem, c_sem, out_sem, ag_send, ag_recv, d_send, d_recv, rs_send, rs_recv,
    s_send, s_recv, a_send, a_recv,
):
    me = tuple(lax.axis_index(name) for name in CLS)
    core = me[3]
    idx = ((me[0] * 4 + me[1]) * 4 + me[2]) * 2 + core
    offset = idx * CLASSES
    place = core * (N // 2) + idx // 2

    def peer(axis, k):
        size = 2 if axis == 3 else 4
        coords = list(me)
        coords[axis] = lax.rem(me[axis] + k, size)
        return tuple(coords)

    def w_copy(i):
        return pltpu.make_async_copy(
            w_hbm.at[pl.ds(i * W_CHUNK, W_CHUNK)],
            E.at[i // 2, pl.ds((i % 2) * 2048, W_CHUNK)],
            w_sem.at[i],
        )

    c_copy = pltpu.make_async_copy(centers_hbm, cen, c_sem)
    for i in range(N_W):
        w_copy(i).start()
    c_copy.start()

    barrier = pltpu.get_barrier_semaphore()
    for axis in range(3):
        for k in (1, 2, 3):
            pl.semaphore_signal(barrier, inc=1, device_id=peer(axis, k), device_id_type=MESH)
    pl.semaphore_signal(barrier, inc=1, device_id=peer(3, 1), device_id_type=MESH)

    acc = jnp.zeros((OWN, D), f32)
    for i in range(N_W):
        w_copy(i).wait()
        acc = acc + plain_dot(
            feat[:, i * W_CHUNK : (i + 1) * W_CHUNK], E[i // 2, (i % 2) * 2048 : (i % 2) * 2048 + W_CHUNK]
        )
    own = acc.astype(bf16).astype(f32)
    own_inv = lax.rsqrt(jnp.sum(own * own, axis=1, keepdims=True) + epsilon)
    own_emb[...] = own
    own_low = (own * own_inv).astype(bf16)

    def put_own(buf, value):
        for p in range(4):
            buf[p, core, me[0], me[1], me[2]] = value[:, p * 128 : (p + 1) * 128]

    def view(buf, p, gathered, at=None):
        at = me if at is None else at
        where = tuple(slice(None) if a in gathered else at[a] for a in range(3))
        return buf.at[(p, core) + where]

    def ag_copy(buf, inst, p, s, k):
        order = ORDERS[p]
        v = view(buf, p, order[:s])
        return pltpu.make_async_remote_copy(
            src_ref=v, dst_ref=v,
            send_sem=ag_send.at[inst, p, s, k - 1], recv_sem=ag_recv.at[inst, p, s, k - 1],
            device_id=peer(order[s], k), device_id_type=MESH,
        )

    def ag_start(buf, inst, s):
        for k in (1, 2, 3):
            for p in range(4):
                ag_copy(buf, inst, p, s, k).start()

    def ag_wait(buf, inst, s):
        for k in (1, 2, 3):
            for p in range(4):
                ag_copy(buf, inst, p, s, k).wait_recv()

    def ag_drain(buf, inst):
        for s in range(3):
            for k in (1, 2, 3):
                for p in range(4):
                    ag_copy(buf, inst, p, s, k).wait_send()

    def pair_copy(buf, inst, p):
        v = buf.at[p, core]
        return pltpu.make_async_remote_copy(
            src_ref=v, dst_ref=v,
            send_sem=d_send.at[inst, p], recv_sem=d_recv.at[inst, p],
            device_id=peer(3, 1), device_id_type=MESH,
        )

    def pair_start(buf, inst):
        for p in range(4):
            pair_copy(buf, inst, p).start()

    def pair_wait(buf, inst):
        for p in range(4):
            pair_copy(buf, inst, p).wait()

    def block(buf, bt):
        c, y0 = bt // 2, (bt % 2) * 2
        return jnp.concatenate([buf[p, c, pl.ds(y0, 2)].reshape(BT, 128) for p in range(4)], axis=1)

    put_own(emb, own_low)
    pl.semaphore_wait(barrier, 10)
    ag_start(emb, 0, 0)

    c_copy.wait()

    @pl.loop(0, CLASSES // JC)
    def _(i):
        r = pl.ds(pl.multiple_of(i * JC, JC), JC)
        cf = cen[r, :].astype(f32)
        inv = lax.rsqrt(jnp.sum(cf * cf, axis=1, keepdims=True) + epsilon)
        low = (cf * inv).astype(bf16)
        clow[r, :] = low
        ct[:, r] = last_dims(eye(D), low).astype(bf16)

    ag_wait(emb, 0, 0)
    ag_start(emb, 0, 1)

    def target_rows(bt):
        lab = labels[pl.ds(bt, 1), :] - offset
        gt[bt] = jnp.zeros((D, BT), f32)

        @pl.loop(0, CLASSES // JB)
        def _(j):
            j0 = pl.multiple_of(j * JB, JB)
            hot = (lab - j0) == lax.broadcasted_iota(jnp.int32, (JB, BT), 0)
            hot = jnp.where(hot, 1.0, 0.0).astype(bf16)
            gt[bt] += plain_dot(ct[:, pl.ds(j0, JB)], hot)

        tt[bt] = gt[bt].astype(bf16)

    @pl.loop(0, 4)
    def _(bt):
        target_rows(bt)

        @pl.when(bt == 0)
        def _():
            ag_wait(emb, 0, 1)
            ag_start(emb, 0, 2)

    ag_wait(emb, 0, 2)
    pair_start(emb, 0)
    pair_wait(emb, 0)

    def tile_of(dev):
        return jnp.minimum((dev * F_DEV) // 128, F // 128 - 2)

    def feature_copy(dev):
        coords = (dev // 32, lax.rem(dev // 8, 4), lax.rem(dev // 2, 4), lax.rem(dev, 2))
        return pltpu.make_async_remote_copy(
            src_ref=feat.at[:, pl.ds(pl.multiple_of(tile_of(dev) * 128, 128), 256)],
            dst_ref=cols.at[place],
            send_sem=a_send, recv_sem=a_recv, device_id=coords, device_id_type=MESH,
        )

    cols[place] = feat[:, pl.ds(pl.multiple_of(tile_of(idx) * 128, 128), 256)]

    @pl.loop(1, N)
    def _(k):
        feature_copy(lax.rem(idx + k, N)).start()

    rows[...] = jnp.zeros_like(rows)

    @pl.loop(0, 4 * (CLASSES // JA))
    def _(i):
        bt, j0 = i // (CLASSES // JA), pl.multiple_of(lax.rem(i, CLASSES // JA) * JA, JA)
        cosines = last_dims(clow[pl.ds(j0, JA), :], block(emb, bt))
        lab = labels[pl.ds(bt, 1), :] - offset - j0
        hot = lab == lax.broadcasted_iota(jnp.int32, (JA, BT), 0)
        e = jnp.where(hot, 0.0, jnp.exp2(cosines * exp2_scale))
        rows[bt] += jnp.sum(e.reshape(JA // 8, 8, BT), axis=0)
        E[bt, pl.ds(j0, JA), :] = e.astype(bf16)

    target = []
    for bt in range(4):
        lab = labels[bt : bt + 1, :] - offset
        here = jnp.logical_and(lab >= 0, lab < CLASSES)
        emb_t = last_dims(eye(D), block(emb, bt))
        tc = jnp.sum(emb_t * tt[bt].astype(f32), axis=0, keepdims=True)
        ts = jnp.sqrt(1.0 - tc * tc)
        margined = logit_scale * (tc * cos_margin - ts * sin_margin)
        slope = cos_margin + sin_margin * tc / ts
        e_t = jnp.where(here, jnp.exp(margined), 0.0)
        slope = jnp.where(here, slope, 0.0)
        target.append((e_t, slope))
        ar_send[0, bt : bt + 1, :] = jnp.sum(rows[bt], axis=0, keepdims=True) + e_t
        ar_send[0, 4 + bt : 5 + bt, :] = jnp.where(here, margined, 0.0)

    AR_AXES = (3, 2, 1, 0)

    def ar_copy(s, k):
        return pltpu.make_async_remote_copy(
            src_ref=ar_send.at[s], dst_ref=ar_recv.at[s, k - 1],
            send_sem=s_send.at[s, k - 1], recv_sem=s_recv.at[s, k - 1],
            device_id=peer(AR_AXES[s], k), device_id_type=MESH,
        )

    def ar_peers(s):
        return (1,) if s == 0 else (1, 2, 3)

    def ar_start(s):
        for k in ar_peers(s):
            ar_copy(s, k).start()

    def ar_finish(s):
        total = ar_send[s]
        for k in ar_peers(s):
            ar_copy(s, k).wait_recv()
            total = total + ar_recv[s, k - 1]
        ar_send[s + 1] = total

    ar_start(0)

    @pl.loop(0, 4)
    def _(bt):
        gt[bt] = jnp.zeros((D, BT), f32)

        @pl.loop(0, CLASSES // JB)
        def _(j):
            j0 = pl.multiple_of(j * JB, JB)
            gt[bt] += plain_dot(ct[:, pl.ds(j0, JB)], E[bt, pl.ds(j0, JB), :])

        for s in range(4):
            @pl.when(bt == s)
            def _():
                ar_finish(s)
                if s < 3:
                    ar_start(s + 1)

    for s in range(4):
        for k in ar_peers(s):
            ar_copy(s, k).wait_send()

    for bt in range(4):
        total = ar_send[4, bt : bt + 1, :]
        loss_out[bt : bt + 1, :] = jnp.log(total) - ar_send[4, 4 + bt : 5 + bt, :]
        e_t, slope = target[bt]
        scale = logit_scale / total
        v = (e_t - total) * slope * scale
        rows[bt, 0:1, :] = scale
        rows[bt, 1:2, :] = v
        g = (gt[bt] * scale + v * tt[bt].astype(f32)).astype(bf16)
        back = last_dims(eye(BT), g).astype(bf16)
        for p in range(4):
            G[p, bt // 2, (bt % 2) * 2 : (bt % 2) * 2 + 2] = back[:, p * 128 : (p + 1) * 128].reshape(2, 4, 4, OWN, 128)

    def rs0_copy(p):
        return pltpu.make_async_remote_copy(
            src_ref=G.at[p, 1 - core], dst_ref=rb0.at[p],
            send_sem=d_send.at[2, p], recv_sem=d_recv.at[2, p],
            device_id=peer(3, 1), device_id_type=MESH,
        )

    def rs_copy(s, p, k):
        order = ORDERS[p]
        axis = order[2 - s]
        to = peer(axis, k)
        if s == 0:
            src = gs.at[(p,) + tuple(to[a] if a == axis else slice(None) for a in range(3))]
            dst = rb1.at[p, k - 1]
        elif s == 1:
            left = sorted(order[:2])
            src = gs2.at[(p,) + tuple(to[a] if a == axis else slice(None) for a in left)]
            dst = rb2.at[p, k - 1]
        else:
            src = gs3.at[p, to[axis]]
            dst = rb3.at[p, k - 1]
        return pltpu.make_async_remote_copy(
            src_ref=src, dst_ref=dst,
            send_sem=rs_send.at[s, p, k - 1], recv_sem=rs_recv.at[s, p, k - 1],
            device_id=to, device_id_type=MESH,
        )

    def rs_start(s):
        for k in (1, 2, 3):
            for p in range(4):
                rs_copy(s, p, k).start()

    def rs_step(stage):
        if stage == 0:
            for p in range(4):
                rs0_copy(p).wait()
                gs[p] = (G[p, core].astype(f32) + rb0[p].astype(f32)).astype(bf16)
            rs_start(0)
            return None
        s = stage - 1
        out = []
        for p in range(4):
            order = ORDERS[p]
            axis = order[2 - s]
            if s == 0:
                total = gs[(p,) + tuple(me[a] if a == axis else slice(None) for a in range(3))]
                bufs = rb1
            elif s == 1:
                total = gs2[(p,) + tuple(me[a] if a == axis else slice(None) for a in sorted(order[:2]))]
                bufs = rb2
            else:
                total = gs3[p, me[axis]]
                bufs = rb3
            total = total.astype(f32)
            for k in (1, 2, 3):
                rs_copy(s, p, k).wait_recv()
                total = total + bufs[p, k - 1].astype(f32)
            if s == 0:
                gs2[p] = total.astype(bf16)
            elif s == 1:
                gs3[p] = total.astype(bf16)
            else:
                out.append(total)
        if s < 2:
            rs_start(s + 1)
            return None
        for s in range(3):
            for p in range(4):
                for k in (1, 2, 3):
                    rs_copy(s, p, k).wait_send()
        return jnp.concatenate(out, axis=1)

    def owner_step():
        grad_dir = rs_step(3)
        own = own_emb[...]
        inv = lax.rsqrt(jnp.sum(own * own, axis=1, keepdims=True) + epsilon)
        direction = own * inv
        along = jnp.sum(grad_dir * direction, axis=1, keepdims=True)
        put_own(gemb, ((grad_dir - direction * along) * inv).astype(bf16))
        ag_start(gemb, 1, 0)

    def ag_step(s):
        ag_wait(gemb, 1, s)
        if s < 2:
            ag_start(gemb, 1, s + 1)
        else:
            pair_start(gemb, 1)

    for p in range(4):
        rs0_copy(p).start()

    def out_copy(i):
        r = pl.ds(pl.multiple_of(i * JC, JC), JC)
        return pltpu.make_async_copy(cen.at[r], gc_hbm.at[r], out_sem.at[i])

    steps = {
        0: functools.partial(rs_step, 0),
        2: functools.partial(rs_step, 1),
        4: functools.partial(rs_step, 2),
        5: owner_step,
        6: functools.partial(ag_step, 0),
        7: functools.partial(ag_step, 1),
    }

    @pl.loop(0, CLASSES // JC)
    def _(i):
        j0 = pl.multiple_of(i * JC, JC)
        r = pl.ds(j0, JC)
        gu = jnp.zeros((JC, D), f32)
        for bt in range(4):
            lab = labels[bt : bt + 1, :] - offset - j0
            hot = lab == lax.broadcasted_iota(jnp.int32, (JC, BT), 0)
            scaled = E[bt, r, :].astype(f32) * rows[bt, 0:1, :]
            gc = jnp.where(hot, rows[bt, 1:2, :], scaled).astype(bf16)
            gu = gu + plain_dot(gc, block(emb, bt))
        cf = cen[r, :].astype(f32)
        inv = lax.rsqrt(jnp.sum(cf * cf, axis=1, keepdims=True) + epsilon)
        cdir = cf * inv
        along = jnp.sum(gu * cdir, axis=1, keepdims=True)
        cen[r, :] = ((gu - cdir * along) * inv).astype(bf16)
        out_copy(i).start()
        for at, step in steps.items():
            @pl.when(i == at)
            def _():
                step()

    ag_step(2)

    others = cols.at[pl.ds(0, N - 1)]
    pltpu.make_async_copy(others, others, a_send).wait()
    pltpu.make_async_copy(others, others, a_recv).wait()

    start = idx * F_DEV - tile_of(idx) * 128
    pick = lax.broadcasted_iota(jnp.int32, (104, 256), 1) == lax.broadcasted_iota(jnp.int32, (104, 256), 0) + start
    pick = pick.astype(f32).astype(bf16)
    mine = [
        last_dims(pick, cols[bt * 32 : (bt + 1) * 32].reshape(BT, 256)).astype(bf16) for bt in range(4)
    ]
    pair_wait(gemb, 1)
    fc = jnp.zeros((104, D), f32)
    for bt in range(4):
        fc = fc + plain_dot(mine[bt], block(gemb, bt))
    fc_out[...] = fc[0:F_DEV]

    for i in range(CLASSES // JC):
        out_copy(i).wait()
    ag_drain(emb, 0)
    ag_drain(gemb, 1)


def on_device(features, fc_weight, centers, labels):
    ordered = labels.reshape(64, 2, OWN).transpose(1, 0, 2).reshape(4, BT)
    vmem = pl.BlockSpec(memory_space=pltpu.VMEM)
    anywhere = pl.BlockSpec(memory_space=pl.ANY)
    dma = pltpu.SemaphoreType.DMA
    loss_all, grad_fc, grad_centers = pl.pallas_call(
        kernel,
        out_shape=(
            jax.ShapeDtypeStruct((4, BT), f32),
            jax.ShapeDtypeStruct((F_DEV, D), f32),
            jax.ShapeDtypeStruct((CLASSES, D), bf16),
        ),
        in_specs=[vmem, anywhere, anywhere, vmem],
        out_specs=(vmem, vmem, anywhere),
        scratch_shapes=[
            pltpu.VMEM((4, CLASSES, BT), bf16),
            pltpu.VMEM((CLASSES, D), bf16),
            pltpu.VMEM((CLASSES, D), bf16),
            pltpu.VMEM((D, CLASSES), bf16),
            pltpu.VMEM((4, D, BT), bf16),
            pltpu.VMEM((4, 2, 4, 4, 4, OWN, 128), bf16),
            pltpu.VMEM((4, 2, 4, 4, 4, OWN, 128), bf16),
            pltpu.VMEM((4, D, BT), f32),
            pltpu.VMEM((4, 2, 4, 4, 4, OWN, 128), bf16),
            pltpu.VMEM((4, 4, 4, 4, OWN, 128), bf16),
            pltpu.VMEM((4, 4, 4, 4, OWN, 128), bf16),
            pltpu.VMEM((4, 3, 4, 4, OWN, 128), bf16),
            pltpu.VMEM((4, 4, 4, OWN, 128), bf16),
            pltpu.VMEM((4, 3, 4, OWN, 128), bf16),
            pltpu.VMEM((4, 4, OWN, 128), bf16),
            pltpu.VMEM((4, 3, OWN, 128), bf16),
            pltpu.VMEM((N, OWN, 256), bf16),
            pltpu.VMEM((OWN, D), f32),
            pltpu.VMEM((5, 8, BT), f32),
            pltpu.VMEM((4, 3, 8, BT), f32),
            pltpu.VMEM((4, 8, BT), f32),
            dma((N_W,)),
            dma,
            dma((CLASSES // JC,)),
            dma((2, 4, 3, 3)),
            dma((2, 4, 3, 3)),
            dma((3, 4)),
            dma((3, 4)),
            dma((3, 4, 3)),
            dma((3, 4, 3)),
            dma((4, 3)),
            dma((4, 3)),
            dma,
            dma,
        ],
        compiler_params=pltpu.CompilerParams(
            collective_id=0, has_side_effects=True, vmem_limit_bytes=66_000_000
        ),
    )(features, fc_weight, centers, ordered)
    position = (lax.axis_index("cls_3") * 64 + lax.axis_index(CLS[:3])) * OWN
    loss = lax.dynamic_slice_in_dim(loss_all.reshape(-1), position, OWN)
    return (loss, grad_centers, grad_fc)


def solution(mesh):
    torus = Mesh(mesh.devices.reshape(4, 4, 4, 2), CLS)
    placed = (P(CLS, None), P(), P(CLS, None), P())
    return jax.shard_map(
        on_device,
        mesh=torus,
        in_specs=placed,
        out_specs=(P(CLS), P(CLS, None), P(CLS, None)),
        check_vma=False,
    )
```

```python
import functools
import math

import jax
import jax.numpy as jnp
from jax import lax
from jax.experimental import pallas as pl
from jax.experimental.pallas import tpu as pltpu
from jax.sharding import Mesh
from jax.sharding import PartitionSpec as P

CLS = ("cls_0", "cls_1", "cls_2", "cls_3")
MESH = pl.DeviceIdType.MESH

logit_scale = 64.0
cos_margin = math.cos(0.5)
sin_margin = math.sin(0.5)
epsilon = 1e-06
exp2_scale = logit_scale / math.log(2.0)

N = 128
D = 512
F = 12544
F_DEV = F // N
OWN = 16
CLASSES = 4096
BT = 512
W_CHUNK = 1792
N_W = F // W_CHUNK
JA = 1024
JB = 2048
JC = 512

ORDERS = ((0, 1, 2), (1, 2, 0), (2, 0, 1), (0, 2, 1))

f32 = jnp.float32
bf16 = jnp.bfloat16


def last_dims(a, b):
    return lax.dot_general(a, b, (((1,), (1,)), ((), ())), preferred_element_type=f32)


def plain_dot(a, b):
    return lax.dot_general(a, b, (((1,), (0,)), ((), ())), preferred_element_type=f32)


def eye(n):
    r = lax.broadcasted_iota(jnp.int32, (n, n), 0)
    c = lax.broadcasted_iota(jnp.int32, (n, n), 1)
    return (r == c).astype(f32).astype(bf16)


def kernel(
    feat, w_hbm, centers_hbm, labels_in,
    loss_out, fc_out, gc_hbm,
    labels,
    E, cen, clow, ct, tt, emb, gemb, gt, G, rb0, gs, rb1, gs2, rb2, gs3, rb3, cols,
    cols_t, fc_send, fc_recv, own_emb, ar_send, ar_recv, rows,
    w_sem, c_sem, out_sem, ag_send, ag_recv, d_send, d_recv, rs_send, rs_recv,
    s_send, s_recv, a_send, a_recv,
):
    me = tuple(lax.axis_index(name) for name in CLS)
    core = me[3]
    idx = ((me[0] * 4 + me[1]) * 4 + me[2]) * 2 + core
    offset = idx * CLASSES
    chip = idx // 2

    def peer(axis, k):
        size = 2 if axis == 3 else 4
        coords = list(me)
        coords[axis] = lax.rem(me[axis] + k, size)
        return tuple(coords)

    def w_copy(i):
        return pltpu.make_async_copy(
            w_hbm.at[pl.ds(i * W_CHUNK, W_CHUNK)],
            E.at[i // 2, pl.ds((i % 2) * 2048, W_CHUNK)],
            w_sem.at[i],
        )

    c_copy = pltpu.make_async_copy(centers_hbm, cen, c_sem)
    for i in range(N_W):
        w_copy(i).start()
    c_copy.start()

    barrier = pltpu.get_barrier_semaphore()
    for axis in range(3):
        for k in (1, 2, 3):
            pl.semaphore_signal(barrier, inc=1, device_id=peer(axis, k), device_id_type=MESH)
    pl.semaphore_signal(barrier, inc=1, device_id=peer(3, 1), device_id_type=MESH)

    lane = lax.broadcasted_iota(jnp.int32, (16, 128), 1)
    for c in range(2):
        low = labels_in[...]
        for m in range(4):
            moved = pltpu.roll(labels_in[...], (-16 * m - 16 * c) % 128, 1)
            low = jnp.where(lane // 16 == m, moved, low)
        high = pltpu.roll(low, 64, 1)
        for g in range(8):
            line = jnp.where(lane[0:1] < 64, low[2 * g : 2 * g + 1], high[2 * g + 1 : 2 * g + 2])
            labels[2 * c + g // 4 : 2 * c + g // 4 + 1, (g % 4) * 128 : (g % 4 + 1) * 128] = line

    acc = jnp.zeros((OWN, D), f32)
    for i in range(N_W):
        w_copy(i).wait()
        acc = acc + plain_dot(
            feat[:, i * W_CHUNK : (i + 1) * W_CHUNK], E[i // 2, (i % 2) * 2048 : (i % 2) * 2048 + W_CHUNK]
        )
    own = acc.astype(bf16).astype(f32)
    own_inv = lax.rsqrt(jnp.sum(own * own, axis=1, keepdims=True) + epsilon)
    own_emb[...] = own
    own_low = (own * own_inv).astype(bf16)

    def put_own(buf, value):
        for p in range(4):
            buf[p, core, me[0], me[1], me[2]] = value[:, p * 128 : (p + 1) * 128]

    def view(buf, p, gathered, at=None):
        at = me if at is None else at
        where = tuple(slice(None) if a in gathered else at[a] for a in range(3))
        return buf.at[(p, core) + where]

    def ag_copy(buf, inst, p, s, k):
        order = ORDERS[p]
        v = view(buf, p, order[:s])
        return pltpu.make_async_remote_copy(
            src_ref=v, dst_ref=v,
            send_sem=ag_send.at[inst, p, s, k - 1], recv_sem=ag_recv.at[inst, p, s, k - 1],
            device_id=peer(order[s], k), device_id_type=MESH,
        )

    def ag_start(buf, inst, p, s):
        for k in (1, 2, 3):
            ag_copy(buf, inst, p, s, k).start()

    def ag_next(buf, inst, s):
        for p in range(4):
            for k in (1, 2, 3):
                ag_copy(buf, inst, p, s, k).wait_recv()
            if s < 2:
                ag_start(buf, inst, p, s + 1)
            elif inst == 0:
                pair_copy(buf, inst, p).start()

    def ag_drain(buf, inst):
        for s in range(3):
            for k in (1, 2, 3):
                for p in range(4):
                    ag_copy(buf, inst, p, s, k).wait_send()

    def pair_copy(buf, inst, p):
        v = buf.at[p, core]
        return pltpu.make_async_remote_copy(
            src_ref=v, dst_ref=v,
            send_sem=d_send.at[inst, p], recv_sem=d_recv.at[inst, p],
            device_id=peer(3, 1), device_id_type=MESH,
        )

    def pair_wait(buf, inst):
        for p in range(4):
            pair_copy(buf, inst, p).wait()

    def block(buf, bt):
        c, y0 = bt // 2, (bt % 2) * 2
        return jnp.concatenate([buf[p, c, pl.ds(y0, 2)].reshape(BT, 128) for p in range(4)], axis=1)

    put_own(emb, own_low)
    pl.semaphore_wait(barrier, 10)
    for p in range(4):
        ag_start(emb, 0, p, 0)

    c_copy.wait()

    @pl.loop(0, CLASSES // JC)
    def _(i):
        r = pl.ds(pl.multiple_of(i * JC, JC), JC)
        cf = cen[r, :].astype(f32)
        inv = lax.rsqrt(jnp.sum(cf * cf, axis=1, keepdims=True) + epsilon)
        low = (cf * inv).astype(bf16)
        clow[r, :] = low
        ct[:, r] = last_dims(eye(D), low).astype(bf16)

    ag_next(emb, 0, 0)

    @pl.loop(0, 4)
    def _(bt):
        lab = labels[pl.ds(bt, 1), :] - offset
        total = jnp.zeros((D, BT), f32)
        for j0 in range(0, CLASSES, JB):
            hot = (lab - j0) == lax.broadcasted_iota(jnp.int32, (JB, BT), 0)
            hot = jnp.where(hot, 1.0, 0.0).astype(bf16)
            total = total + plain_dot(ct[:, j0 : j0 + JB], hot)
        tt[bt] = total.astype(bf16)

        @pl.when(bt == 0)
        def _():
            ag_next(emb, 0, 1)

    ag_next(emb, 0, 2)

    def tile_of(c):
        return jnp.minimum((c * 2 * F_DEV) // 128, F // 128 - 3)

    def feature_copy(k):
        to = lax.bitwise_and(chip + k, N // 2 - 1)
        coords = (
            lax.shift_right_logical(to, 4), lax.bitwise_and(lax.shift_right_logical(to, 2), 3), lax.bitwise_and(to, 3), core
        )
        return pltpu.make_async_remote_copy(
            src_ref=feat.at[:, pl.ds(pl.multiple_of(tile_of(to) * 128, 128), 384)],
            dst_ref=cols.at[chip],
            send_sem=a_send, recv_sem=a_recv, device_id=coords, device_id_type=MESH,
        )

    cols[chip] = feat[:, pl.ds(pl.multiple_of(tile_of(chip) * 128, 128), 384)]

    rows[...] = jnp.zeros_like(rows)
    n_a = CLASSES // JA
    tiles = 4 * n_a

    def tile_at(t):
        bt = lax.rem(t // n_a + 2 * core, 4)
        return bt, pl.multiple_of(lax.rem(t, n_a) * JA, JA)

    def cosine_tile(t, slot):
        bt, j0 = tile_at(t)
        gt[2 * slot : 2 * slot + 2] = last_dims(clow[pl.ds(j0, JA), :], block(emb, bt)).reshape(2, BT, BT)

    def exp_tile(t, slot):
        bt, j0 = tile_at(t)
        cosines = gt[2 * slot : 2 * slot + 2].reshape(JA, BT)
        lab = labels[pl.ds(bt, 1), :] - offset - j0
        hot = lab == lax.broadcasted_iota(jnp.int32, (JA, BT), 0)
        e = jnp.where(hot, 0.0, jnp.exp2(cosines * exp2_scale))
        rows[bt] += jnp.sum(e.reshape(JA // 8, 8, BT), axis=0)
        E[bt, pl.ds(j0, JA), :] = e.astype(bf16)

    cosine_tile(0, 0)

    @pl.loop(0, tiles // 2 - 1)
    def _(m):
        @pl.when(m == tiles // 4 - 1)
        def _():
            pair_wait(emb, 0)

        for u in range(9):
            feature_copy(m * 9 + u + 1).start()
        cosine_tile(2 * m + 1, 1)
        exp_tile(2 * m, 0)
        cosine_tile(2 * m + 2, 0)
        exp_tile(2 * m + 1, 1)

    cosine_tile(tiles - 1, 1)
    exp_tile(tiles - 2, 0)
    exp_tile(tiles - 1, 1)

    target = []
    for bt in range(4):
        lab = labels[bt : bt + 1, :] - offset
        here = jnp.logical_and(lab >= 0, lab < CLASSES)
        emb_t = last_dims(eye(D), block(emb, bt))
        tc = jnp.sum(emb_t * tt[bt].astype(f32), axis=0, keepdims=True)
        ts = jnp.sqrt(1.0 - tc * tc)
        margined = logit_scale * (tc * cos_margin - ts * sin_margin)
        slope = cos_margin + sin_margin * tc / ts
        e_t = jnp.where(here, jnp.exp(margined), 0.0)
        slope = jnp.where(here, slope, 0.0)
        target.append((e_t, slope))
        ar_send[0, bt : bt + 1, :] = jnp.sum(rows[bt], axis=0, keepdims=True) + e_t
        ar_send[0, 4 + bt : 5 + bt, :] = jnp.where(here, margined, 0.0)

    AR_AXES = (3, 2, 1, 0)

    def ar_copy(s, k):
        return pltpu.make_async_remote_copy(
            src_ref=ar_send.at[s], dst_ref=ar_recv.at[s, k - 1],
            send_sem=s_send.at[s, k - 1], recv_sem=s_recv.at[s, k - 1],
            device_id=peer(AR_AXES[s], k), device_id_type=MESH,
        )

    def ar_peers(s):
        return (1,) if s == 0 else (1, 2, 3)

    def ar_start(s):
        for k in ar_peers(s):
            ar_copy(s, k).start()

    def ar_finish(s):
        total = ar_send[s]
        for k in ar_peers(s):
            ar_copy(s, k).wait_recv()
            total = total + ar_recv[s, k - 1]
        ar_send[s + 1] = total

    ar_start(0)

    @pl.loop(0, 4)
    def _(i):
        bt = lax.rem(i + 2 * core + 2, 4)
        for h in range(CLASSES // JB):
            part = plain_dot(ct[:, h * JB : (h + 1) * JB], E[bt, h * JB : (h + 1) * JB, :])
            gt[bt] = part if h == 0 else gt[bt] + part
        for s in range(4):
            @pl.when(i == s)
            def _():
                ar_finish(s)
                if s < 3:
                    ar_start(s + 1)

    for s in range(4):
        for k in ar_peers(s):
            ar_copy(s, k).wait_send()

    for bt in range(4):
        total = ar_send[4, bt : bt + 1, :]
        loss_out[bt : bt + 1, :] = jnp.log(total) - ar_send[4, 4 + bt : 5 + bt, :]
        e_t, slope = target[bt]
        scale = logit_scale / total
        v = (e_t - total) * slope * scale
        rows[bt, 0:1, :] = scale
        rows[bt, 1:2, :] = v
        g = (gt[bt] * scale + v * tt[bt].astype(f32)).astype(bf16)
        back = last_dims(eye(BT), g).astype(bf16)
        for p in range(4):
            G[p, bt // 2, (bt % 2) * 2 : (bt % 2) * 2 + 2] = back[:, p * 128 : (p + 1) * 128].reshape(2, 4, 4, OWN, 128)

    def rs0_copy(p):
        return pltpu.make_async_remote_copy(
            src_ref=G.at[p, 1 - core], dst_ref=rb0.at[p],
            send_sem=d_send.at[2, p], recv_sem=d_recv.at[2, p],
            device_id=peer(3, 1), device_id_type=MESH,
        )

    def rs_copy(s, p, k):
        order = ORDERS[p]
        axis = order[2 - s]
        to = peer(axis, k)
        if s == 0:
            src = gs.at[(p,) + tuple(to[a] if a == axis else slice(None) for a in range(3))]
            dst = rb1.at[p, k - 1]
        elif s == 1:
            left = sorted(order[:2])
            src = gs2.at[(p,) + tuple(to[a] if a == axis else slice(None) for a in left)]
            dst = rb2.at[p, k - 1]
        else:
            src = gs3.at[p, to[axis]]
            dst = rb3.at[p, k - 1]
        return pltpu.make_async_remote_copy(
            src_ref=src, dst_ref=dst,
            send_sem=rs_send.at[s, p, k - 1], recv_sem=rs_recv.at[s, p, k - 1],
            device_id=to, device_id_type=MESH,
        )

    def rs_start(s, p):
        for k in (1, 2, 3):
            rs_copy(s, p, k).start()

    def rs_step(stage):
        if stage == 0:
            for p in range(4):
                rs0_copy(p).wait()
                gs[p] = (G[p, core].astype(f32) + rb0[p].astype(f32)).astype(bf16)
                rs_start(0, p)
            return None
        s = stage - 1
        out = []
        for p in range(4):
            order = ORDERS[p]
            axis = order[2 - s]
            if s == 0:
                total = gs[(p,) + tuple(me[a] if a == axis else slice(None) for a in range(3))]
                bufs = rb1
            elif s == 1:
                total = gs2[(p,) + tuple(me[a] if a == axis else slice(None) for a in sorted(order[:2]))]
                bufs = rb2
            else:
                total = gs3[p, me[axis]]
                bufs = rb3
            total = total.astype(f32)
            for k in (1, 2, 3):
                rs_copy(s, p, k).wait_recv()
                total = total + bufs[p, k - 1].astype(f32)
            if s == 0:
                gs2[p] = total.astype(bf16)
                rs_start(1, p)
            elif s == 1:
                gs3[p] = total.astype(bf16)
                rs_start(2, p)
            else:
                out.append(total)
        if s < 2:
            return None
        for s in range(3):
            for p in range(4):
                for k in (1, 2, 3):
                    rs_copy(s, p, k).wait_send()
        return jnp.concatenate(out, axis=1)

    def owner_step():
        grad_dir = rs_step(3)
        own = own_emb[...]
        inv = lax.rsqrt(jnp.sum(own * own, axis=1, keepdims=True) + epsilon)
        direction = own * inv
        along = jnp.sum(grad_dir * direction, axis=1, keepdims=True)
        put_own(gemb, ((grad_dir - direction * along) * inv).astype(bf16))
        for p in range(4):
            ag_start(gemb, 1, p, 0)

    for p in range(4):
        rs0_copy(p).start()

    def out_copy(i):
        r = pl.ds(pl.multiple_of(i * JC, JC), JC)
        return pltpu.make_async_copy(clow.at[r], gc_hbm.at[r], out_sem.at[i])

    steps = {
        0: functools.partial(rs_step, 0),
        2: functools.partial(rs_step, 1),
        4: functools.partial(rs_step, 2),
        5: owner_step,
        6: functools.partial(ag_next, gemb, 1, 0),
        7: functools.partial(ag_next, gemb, 1, 1),
    }

    def finish_centers(i, slot):
        r = pl.ds(pl.multiple_of(i * JC, JC), JC)
        gu = gt[slot]
        cf = cen[r, :].astype(f32)
        inv = lax.rsqrt(jnp.sum(cf * cf, axis=1, keepdims=True) + epsilon)
        along = jnp.sum(gu * cf, axis=1, keepdims=True) * (inv * inv * inv)
        clow[r, :] = (gu * inv - cf * along).astype(bf16)

    @pl.loop(0, CLASSES // JC)
    def _(i):
        j0 = pl.multiple_of(i * JC, JC)
        r = pl.ds(j0, JC)
        gu = jnp.zeros((JC, D), f32)
        for bt in range(4):
            lab = labels[bt : bt + 1, :] - offset - j0
            hot = lab == lax.broadcasted_iota(jnp.int32, (JC, BT), 0)
            scaled = E[bt, r, :].astype(f32) * rows[bt, 0:1, :]
            gc = jnp.where(hot, rows[bt, 1:2, :], scaled).astype(bf16)
            gu = gu + plain_dot(gc, block(emb, bt))
        gt[lax.rem(i, 2)] = gu
        before = jnp.maximum(i - 1, 0)
        finish_centers(before, lax.rem(i + 1, 2))

        @pl.when(i > 0)
        def _():
            out_copy(before).start()

        for at, step in steps.items():
            @pl.when(i == at)
            def _():
                step()

    finish_centers(CLASSES // JC - 1, (CLASSES // JC - 1) % 2)
    out_copy(CLASSES // JC - 1).start()

    others = cols.at[pl.ds(0, N // 2 - 1)]
    pltpu.make_async_copy(others, others, a_send).wait()
    pltpu.make_async_copy(others, others, a_recv).wait()

    start = chip * 2 * F_DEV - tile_of(chip) * 128
    r = lax.broadcasted_iota(jnp.int32, (208, 384), 0)
    want = start + jnp.where(r < 104, core * F_DEV + r, (1 - core) * F_DEV + r - 104)
    pick = (lax.broadcasted_iota(jnp.int32, (208, 384), 1) == want).astype(f32).astype(bf16)
    for h in range(2):
        cols_t[h] = last_dims(pick, cols[h * 32 : (h + 1) * 32].reshape(BT, 384)).astype(bf16)

    ag_next(gemb, 1, 2)
    fc = jnp.zeros((208, D), f32)
    for h in range(2):
        rows_h = jnp.concatenate([gemb[p, core, 2 * h : 2 * h + 2].reshape(BT, 128) for p in range(4)], axis=1)
        fc = fc + plain_dot(cols_t[h], rows_h)
    fc_send[...] = fc[104:208]
    fc_copy = pltpu.make_async_remote_copy(
        src_ref=fc_send, dst_ref=fc_recv, send_sem=d_send.at[1, 0], recv_sem=d_recv.at[1, 0],
        device_id=peer(3, 1), device_id_type=MESH,
    )
    fc_copy.start()
    fc_copy.wait()
    fc_out[...] = (fc[0:104] + fc_recv[...])[0:F_DEV]

    for i in range(CLASSES // JC):
        out_copy(i).wait()
    ag_drain(emb, 0)
    ag_drain(gemb, 1)


def emit_kernel(loss_all, fc, gc_hbm, loss_out, fc_out, out_hbm, held, in_sem, out_sem):
    step = CLASSES // 8

    def read(i):
        r = pl.ds(i * step, step)
        return pltpu.make_async_copy(gc_hbm.at[r], held.at[r], in_sem.at[i])

    def write(i):
        r = pl.ds(i * step, step)
        return pltpu.make_async_copy(held.at[r], out_hbm.at[r], out_sem.at[i])

    for i in range(8):
        read(i).start()
    chip = (lax.axis_index("cls_0") * 4 + lax.axis_index("cls_1")) * 4 + lax.axis_index("cls_2")
    position = lax.axis_index("cls_3") * 64 + chip
    line = loss_all[pl.ds(position // 32, 1), :]
    loss_out[...] = pltpu.roll(line, lax.rem(BT - lax.rem(position, 32) * OWN, BT), 1)[:, 0:OWN]
    fc_out[...] = fc[...]
    for i in range(8):
        read(i).wait()
        write(i).start()
    for i in range(8):
        write(i).wait()


def on_device(features, fc_weight, centers, labels):
    vmem = pl.BlockSpec(memory_space=pltpu.VMEM)
    anywhere = pl.BlockSpec(memory_space=pl.ANY)
    dma = pltpu.SemaphoreType.DMA
    loss_all, grad_fc, grad_centers = pl.pallas_call(
        kernel,
        out_shape=(
            jax.ShapeDtypeStruct((4, BT), f32),
            jax.ShapeDtypeStruct((F_DEV, D), f32),
            jax.ShapeDtypeStruct((CLASSES, D), bf16),
        ),
        in_specs=[vmem, anywhere, anywhere, vmem],
        out_specs=(vmem, vmem, anywhere),
        scratch_shapes=[
            pltpu.VMEM((4, BT), jnp.int32),
            pltpu.VMEM((4, CLASSES, BT), bf16),
            pltpu.VMEM((CLASSES, D), bf16),
            pltpu.VMEM((CLASSES, D), bf16),
            pltpu.VMEM((D, CLASSES), bf16),
            pltpu.VMEM((4, D, BT), bf16),
            pltpu.VMEM((4, 2, 4, 4, 4, OWN, 128), bf16),
            pltpu.VMEM((4, 2, 4, 4, 4, OWN, 128), bf16),
            pltpu.VMEM((4, D, BT), f32),
            pltpu.VMEM((4, 2, 4, 4, 4, OWN, 128), bf16),
            pltpu.VMEM((4, 4, 4, 4, OWN, 128), bf16),
            pltpu.VMEM((4, 4, 4, 4, OWN, 128), bf16),
            pltpu.VMEM((4, 3, 4, 4, OWN, 128), bf16),
            pltpu.VMEM((4, 4, 4, OWN, 128), bf16),
            pltpu.VMEM((4, 3, 4, OWN, 128), bf16),
            pltpu.VMEM((4, 4, OWN, 128), bf16),
            pltpu.VMEM((4, 3, OWN, 128), bf16),
            pltpu.VMEM((N // 2, OWN, 384), bf16),
            pltpu.VMEM((2, 208, BT), bf16),
            pltpu.VMEM((104, D), f32),
            pltpu.VMEM((104, D), f32),
            pltpu.VMEM((OWN, D), f32),
            pltpu.VMEM((5, 8, BT), f32),
            pltpu.VMEM((4, 3, 8, BT), f32),
            pltpu.VMEM((4, 8, BT), f32),
            dma((N_W,)),
            dma,
            dma((CLASSES // JC,)),
            dma((2, 4, 3, 3)),
            dma((2, 4, 3, 3)),
            dma((3, 4)),
            dma((3, 4)),
            dma((3, 4, 3)),
            dma((3, 4, 3)),
            dma((4, 3)),
            dma((4, 3)),
            dma,
            dma,
        ],
        compiler_params=pltpu.CompilerParams(
            collective_id=0, has_side_effects=True, vmem_limit_bytes=66_000_000
        ),
    )(features, fc_weight, centers, labels.reshape(16, 128))
    loss, grad_fc, grad_centers = pl.pallas_call(
        emit_kernel,
        out_shape=(
            jax.ShapeDtypeStruct((1, OWN), f32),
            jax.ShapeDtypeStruct((F_DEV, D), f32),
            jax.ShapeDtypeStruct((CLASSES, D), bf16),
        ),
        in_specs=[vmem, vmem, anywhere],
        out_specs=(vmem, vmem, anywhere),
        scratch_shapes=[pltpu.VMEM((CLASSES, D), bf16), dma((8,)), dma((8,))],
    )(loss_all, grad_fc, grad_centers)
    return (loss.reshape(-1), grad_centers, grad_fc)


def solution(mesh):
    torus = Mesh(mesh.devices.reshape(4, 4, 4, 2), CLS)
    placed = (P(CLS, None), P(), P(CLS, None), P())
    return jax.shard_map(
        on_device,
        mesh=torus,
        in_specs=placed,
        out_specs=(P(CLS), P(CLS, None), P(CLS, None)),
        check_vma=False,
    )
```

```python
import functools
import math

import jax
import jax.numpy as jnp
from jax import lax
from jax.experimental import pallas as pl
from jax.experimental.pallas import tpu as pltpu
from jax.sharding import Mesh
from jax.sharding import PartitionSpec as P

CLS = ("cls_0", "cls_1", "cls_2", "cls_3")
MESH = pl.DeviceIdType.MESH

logit_scale = 64.0
cos_margin = math.cos(0.5)
sin_margin = math.sin(0.5)
epsilon = 1e-06
exp2_scale = logit_scale / math.log(2.0)

N = 128
D = 512
F = 12544
F_DEV = F // N
OWN = 16
CLASSES = 4096
BT = 512
W_CHUNK = 1792
N_W = F // W_CHUNK
JA = 1024
JB = 2048
JC = 512

ORDERS = ((0, 1, 2), (1, 2, 0), (2, 0, 1), (0, 2, 1), (0, 1, 2))

f32 = jnp.float32
bf16 = jnp.bfloat16


def last_dims(a, b):
    return lax.dot_general(a, b, (((1,), (1,)), ((), ())), preferred_element_type=f32)


def plain_dot(a, b):
    return lax.dot_general(a, b, (((1,), (0,)), ((), ())), preferred_element_type=f32)


def transposed(x):
    width = x.shape[1]
    one = eye(256)
    return jnp.concatenate([last_dims(one, x[:, c : c + 256]) for c in range(0, width, 256)], axis=0).astype(bf16)


def eye(n):
    r = lax.broadcasted_iota(jnp.int32, (n, n), 0)
    c = lax.broadcasted_iota(jnp.int32, (n, n), 1)
    return (r == c).astype(f32).astype(bf16)


def kernel(
    feat, w_hbm, centers_hbm, labels_in,
    loss_out, fc_out, gc_hbm,
    labels,
    E, cen, clow, ct, tt, ttr, emb, gemb, gt, gsend, grecv, gs, rb1, gs2, rb2, gs3, rb3, rs_out, cols,
    cols_t, fc_send, fc_recv, own_emb, ar_send, ar_recv, rows,
    w_sem, c_sem, out_sem, ag_send, ag_recv, d_send, d_recv, rs_send, rs_recv,
    s_send, s_recv, a_send, a_recv,
):
    me = tuple(lax.axis_index(name) for name in CLS)
    core = me[3]
    idx = ((me[0] * 4 + me[1]) * 4 + me[2]) * 2 + core
    offset = idx * CLASSES
    chip = idx // 2

    def peer(axis, k):
        size = 2 if axis == 3 else 4
        coords = list(me)
        coords[axis] = lax.rem(me[axis] + k, size)
        return tuple(coords)

    def w_copy(i):
        return pltpu.make_async_copy(
            w_hbm.at[pl.ds(i * W_CHUNK, W_CHUNK)],
            E.at[i // 2, pl.ds((i % 2) * 2048, W_CHUNK)],
            w_sem.at[i],
        )

    c_copy = pltpu.make_async_copy(centers_hbm, cen, c_sem)
    for i in range(N_W):
        w_copy(i).start()
    c_copy.start()

    barrier = pltpu.get_barrier_semaphore()
    for axis in range(3):
        for k in (1, 2, 3):
            pl.semaphore_signal(barrier, inc=1, device_id=peer(axis, k), device_id_type=MESH)
    pl.semaphore_signal(barrier, inc=1, device_id=peer(3, 1), device_id_type=MESH)

    lane = lax.broadcasted_iota(jnp.int32, (16, 128), 1)
    for c in range(2):
        low = labels_in[...]
        for m in range(4):
            moved = pltpu.roll(labels_in[...], (-16 * m - 16 * c) % 128, 1)
            low = jnp.where(lane // 16 == m, moved, low)
        high = pltpu.roll(low, 64, 1)
        for g in range(8):
            line = jnp.where(lane[0:1] < 64, low[2 * g : 2 * g + 1], high[2 * g + 1 : 2 * g + 2])
            labels[2 * c + g // 4 : 2 * c + g // 4 + 1, (g % 4) * 128 : (g % 4 + 1) * 128] = line

    acc = jnp.zeros((OWN, D), f32)
    for i in range(N_W):
        w_copy(i).wait()
        acc = acc + plain_dot(
            feat[:, i * W_CHUNK : (i + 1) * W_CHUNK], E[i // 2, (i % 2) * 2048 : (i % 2) * 2048 + W_CHUNK]
        )
    own = acc.astype(bf16).astype(f32)
    own_inv = lax.rsqrt(jnp.sum(own * own, axis=1, keepdims=True) + epsilon)
    own_emb[...] = own
    own_low = (own * own_inv).astype(bf16)

    def put_own(buf, value):
        for p in range(4):
            buf[p, core, me[0], me[1], me[2]] = value[:, p * 128 : (p + 1) * 128]

    def view(buf, p, gathered, at=None):
        at = me if at is None else at
        where = tuple(slice(None) if a in gathered else at[a] for a in range(3))
        return buf.at[(p, core) + where]

    def by_order(p, act):
        if p < 3:
            act(ORDERS[p])
            return
        for c in range(2):
            @pl.when(core == c)
            def _():
                act(ORDERS[3 + c])

    def ag_copy(buf, inst, p, s, k, order):
        v = view(buf, p, order[:s])
        return pltpu.make_async_remote_copy(
            src_ref=v, dst_ref=v,
            send_sem=ag_send.at[inst, p, s, k - 1], recv_sem=ag_recv.at[inst, p, s, k - 1],
            device_id=peer(order[s], k), device_id_type=MESH,
        )

    def ag_start(buf, inst, p, s):
        def act(order):
            for k in (1, 2, 3):
                ag_copy(buf, inst, p, s, k, order).start()

        by_order(p, act)

    def ag_next(buf, inst, s):
        for p in range(4):
            for k in (1, 2, 3):
                ag_copy(buf, inst, p, s, k, ORDERS[p]).wait_recv()
            if s < 2:
                ag_start(buf, inst, p, s + 1)
            elif inst == 0:
                pair_copy(buf, inst, p).start()

    def ag_drain(buf, inst):
        for s in range(3):
            for k in (1, 2, 3):
                for p in range(4):
                    ag_copy(buf, inst, p, s, k, ORDERS[p]).wait_send()

    def pair_copy(buf, inst, p):
        v = buf.at[p, core]
        return pltpu.make_async_remote_copy(
            src_ref=v, dst_ref=v,
            send_sem=d_send.at[inst, p], recv_sem=d_recv.at[inst, p],
            device_id=peer(3, 1), device_id_type=MESH,
        )

    def pair_wait(buf, inst):
        for p in range(4):
            pair_copy(buf, inst, p).wait()

    def block(buf, bt):
        c, y0 = bt // 2, (bt % 2) * 2
        return jnp.concatenate([buf[p, c, pl.ds(y0, 2)].reshape(BT, 128) for p in range(4)], axis=1)

    put_own(emb, own_low)
    pl.semaphore_wait(barrier, 10)
    for p in range(4):
        ag_start(emb, 0, p, 0)

    c_copy.wait()

    @pl.loop(0, CLASSES // JC)
    def _(i):
        r = pl.ds(pl.multiple_of(i * JC, JC), JC)
        cf = cen[r, :].astype(f32)
        inv = lax.rsqrt(jnp.sum(cf * cf, axis=1, keepdims=True) + epsilon)
        low = (cf * inv).astype(bf16)
        clow[r, :] = low
        ct[:, r] = transposed(low)

        @pl.when(i == 4)
        def _():
            ag_next(emb, 0, 0)

    @pl.loop(0, 4)
    def _(bt):
        lab = labels[pl.ds(bt, 1), :] - offset
        total = jnp.zeros((D, BT), f32)
        for j0 in range(0, CLASSES, JB):
            hot = (lab - j0) == lax.broadcasted_iota(jnp.int32, (JB, BT), 0)
            hot = jnp.where(hot, 1.0, 0.0).astype(bf16)
            total = total + plain_dot(ct[:, j0 : j0 + JB], hot)
        tt[bt] = total.astype(bf16)

        @pl.when(bt == 0)
        def _():
            ag_next(emb, 0, 1)

    ag_next(emb, 0, 2)

    def tt_copy():
        return pltpu.make_async_remote_copy(
            src_ref=tt.at[pl.ds(2 * (1 - core), 2)], dst_ref=ttr,
            send_sem=d_send.at[1, 1], recv_sem=d_recv.at[1, 1], device_id=peer(3, 1), device_id_type=MESH,
        )

    tt_copy().start()
    def tile_of(c):
        return jnp.minimum((c * 2 * F_DEV) // 128, F // 128 - 3)

    def feature_copy(k):
        to = lax.bitwise_and(chip + k, N // 2 - 1)
        coords = (
            lax.shift_right_logical(to, 4), lax.bitwise_and(lax.shift_right_logical(to, 2), 3), lax.bitwise_and(to, 3), core
        )
        return pltpu.make_async_remote_copy(
            src_ref=feat.at[:, pl.ds(pl.multiple_of(tile_of(to) * 128, 128), 384)],
            dst_ref=cols.at[chip],
            send_sem=a_send, recv_sem=a_recv, device_id=coords, device_id_type=MESH,
        )

    cols[chip] = feat[:, pl.ds(pl.multiple_of(tile_of(chip) * 128, 128), 384)]

    rows[...] = jnp.zeros_like(rows)
    n_a = CLASSES // JA
    tiles = 4 * n_a

    def tile_at(t):
        bt = lax.rem(t // n_a + 2 * core, 4)
        return bt, pl.multiple_of(lax.rem(t, n_a) * JA, JA)

    def cosine_tile(t, slot):
        bt, j0 = tile_at(t)
        gt[2 * slot : 2 * slot + 2] = last_dims(clow[pl.ds(j0, JA), :], block(emb, bt)).reshape(2, BT, BT)

    def exp_tile(t, slot):
        bt, j0 = tile_at(t)
        cosines = gt[2 * slot : 2 * slot + 2].reshape(JA, BT)
        lab = labels[pl.ds(bt, 1), :] - offset - j0
        hot = lab == lax.broadcasted_iota(jnp.int32, (JA, BT), 0)
        e = jnp.where(hot, 0.0, jnp.exp2(cosines * exp2_scale))
        rows[bt] += jnp.sum(e.reshape(JA // 8, 8, BT), axis=0)
        E[bt, pl.ds(j0, JA), :] = e.astype(bf16)

    cosine_tile(0, 0)

    @pl.loop(0, tiles // 2 - 1)
    def _(m):
        @pl.when(m == tiles // 4 - 1)
        def _():
            pair_wait(emb, 0)

        for u in range(9):
            feature_copy(m * 9 + u + 1).start()
        cosine_tile(2 * m + 1, 1)
        exp_tile(2 * m, 0)
        cosine_tile(2 * m + 2, 0)
        exp_tile(2 * m + 1, 1)

    cosine_tile(tiles - 1, 1)
    exp_tile(tiles - 2, 0)
    exp_tile(tiles - 1, 1)

    def margin(tc):
        ts = jnp.sqrt(1.0 - tc * tc)
        margined = logit_scale * (tc * cos_margin - ts * sin_margin)
        return margined, cos_margin + sin_margin * tc / ts

    def on_chip(bt):
        lab = labels[pl.ds(bt, 1), :] - chip * (2 * CLASSES)
        return jnp.logical_and(lab >= 0, lab < 2 * CLASSES)

    ar_send[0, 4:8, :] = jnp.zeros((4, BT), f32)
    for bt in range(4):
        ar_send[0, bt : bt + 1, :] = jnp.sum(rows[bt], axis=0, keepdims=True)
    tt_copy().wait()
    for h in range(2):
        bt = 2 * core + h
        rows_t = tt[bt].astype(f32) + ttr[h].astype(f32)
        ttr[h] = rows_t.astype(bf16)
        own_rows = jnp.concatenate([emb[p, core, 2 * h : 2 * h + 2].reshape(BT, 128) for p in range(4)], axis=1)
        tc = jnp.sum(transposed(own_rows).astype(f32) * rows_t, axis=0, keepdims=True)
        margined, _ = margin(tc)
        ar_send[0, pl.ds(bt, 1), :] += jnp.where(on_chip(bt), jnp.exp(margined), 0.0)
        ar_send[0, pl.ds(4 + bt, 1), :] = tc

    AR_PEERS = (
        tuple((z, c) for z in range(4) for c in range(2) if z + c > 0),
        tuple((1, k) for k in (1, 2, 3)),
        tuple((0, k) for k in (1, 2, 3)),
    )

    def ar_copy(s, n):
        if s == 0:
            dz, dc = AR_PEERS[0][n]
            to = (me[0], me[1], lax.rem(me[2] + dz, 4), lax.rem(core + dc, 2))
        else:
            to = peer(*AR_PEERS[s][n])
        return pltpu.make_async_remote_copy(
            src_ref=ar_send.at[s], dst_ref=ar_recv.at[s, n],
            send_sem=s_send.at[s, n], recv_sem=s_recv.at[s, n],
            device_id=to, device_id_type=MESH,
        )

    def ar_start(s):
        for n in range(len(AR_PEERS[s])):
            ar_copy(s, n).start()

    def ar_finish(s):
        total = ar_send[s]
        for n in range(len(AR_PEERS[s])):
            ar_copy(s, n).wait_recv()
            total = total + ar_recv[s, n]
        ar_send[s + 1] = total
        if s < 2:
            ar_start(s + 1)

    ar_start(0)

    def g_copy(h):
        return pltpu.make_async_remote_copy(
            src_ref=gsend.at[h], dst_ref=grecv.at[h],
            send_sem=d_send.at[2, h], recv_sem=d_recv.at[2, h], device_id=peer(3, 1), device_id_type=MESH,
        )

    half = CLASSES // 2

    @pl.loop(0, 4)
    def _(i):
        bt = lax.rem(i + 2 * core + 2, 4)
        gt[i] = plain_dot(ct[:, 0:half], E[bt, 0:half, :])

        @pl.when(i == 1)
        def _():
            ar_finish(0)

        gt[i] += plain_dot(ct[:, half:], E[bt, half:, :])

        @pl.when(i == 2)
        def _():
            ar_finish(1)

        @pl.when(i < 2)
        def _():
            gsend[i] = gt[i].astype(bf16)
            g_copy(i).start()

    ar_finish(2)
    for s in range(3):
        for n in range(len(AR_PEERS[s])):
            ar_copy(s, n).wait_send()

    for bt in range(4):
        total = ar_send[3, bt : bt + 1, :]
        margined, slope = margin(ar_send[3, 4 + bt : 5 + bt, :])
        loss_out[bt : bt + 1, :] = jnp.log(total) - margined
        scale = logit_scale / total
        rows[bt, 0:1, :] = scale
        rows[bt, 1:2, :] = (jnp.exp(margined) - total) * slope * scale

    for h in range(2):
        bt = 2 * core + h
        g_copy(h).wait()
        v = jnp.where(on_chip(bt), rows[bt, 1:2, :], 0.0)
        g = (gt[2 + h] + grecv[h].astype(f32)) * rows[bt, 0:1, :] + v * ttr[h].astype(f32)
        back = transposed(g.astype(bf16))
        for p in range(4):
            gs[p, 2 * h : 2 * h + 2] = back[:, p * 128 : (p + 1) * 128].reshape(2, 4, 4, OWN, 128)

    def rs_copy(s, p, k, order):
        axis = order[2 - s]
        to = peer(axis, k)
        if s == 0:
            src = gs.at[(p,) + tuple(to[a] if a == axis else slice(None) for a in range(3))]
            dst = rb1.at[p, k - 1]
        elif s == 1:
            left = sorted(order[:2])
            src = gs2.at[(p,) + tuple(to[a] if a == axis else slice(None) for a in left)]
            dst = rb2.at[p, k - 1]
        else:
            src = gs3.at[p, to[axis]]
            dst = rb3.at[p, k - 1]
        return pltpu.make_async_remote_copy(
            src_ref=src, dst_ref=dst,
            send_sem=rs_send.at[s, p, k - 1], recv_sem=rs_recv.at[s, p, k - 1],
            device_id=to, device_id_type=MESH,
        )

    def rs_start(s, p):
        def act(order):
            for k in (1, 2, 3):
                rs_copy(s, p, k, order).start()

        by_order(p, act)

    def rs_step(s):
        bufs = (rb1, rb2, rb3)[s]
        for p in range(4):
            for k in (1, 2, 3):
                rs_copy(s, p, k, ORDERS[p]).wait_recv()

            def act(order):
                axis = order[2 - s]
                if s == 0:
                    total = gs[(p,) + tuple(me[a] if a == axis else slice(None) for a in range(3))]
                elif s == 1:
                    total = gs2[(p,) + tuple(me[a] if a == axis else slice(None) for a in sorted(order[:2]))]
                else:
                    total = gs3[p, me[axis]]
                total = total.astype(f32)
                for k in (1, 2, 3):
                    total = total + bufs[p, k - 1].astype(f32)
                if s == 0:
                    gs2[p] = total.astype(bf16)
                elif s == 1:
                    gs3[p] = total.astype(bf16)
                else:
                    rs_out[:, p * 128 : (p + 1) * 128] = total
                if s < 2:
                    for k in (1, 2, 3):
                        rs_copy(s + 1, p, k, order).start()

            by_order(p, act)

    def owner_step():
        rs_step(2)
        grad_dir = rs_out[...]
        own = own_emb[...]
        inv = lax.rsqrt(jnp.sum(own * own, axis=1, keepdims=True) + epsilon)
        direction = own * inv
        along = jnp.sum(grad_dir * direction, axis=1, keepdims=True)
        put_own(gemb, ((grad_dir - direction * along) * inv).astype(bf16))
        for p in range(4):
            ag_start(gemb, 1, p, 0)

    for p in range(4):
        rs_start(0, p)

    def out_copy(i):
        r = pl.ds(pl.multiple_of(i * JC, JC), JC)
        return pltpu.make_async_copy(clow.at[r], gc_hbm.at[r], out_sem.at[i])

    steps = {
        3: functools.partial(rs_step, 0),
        5: functools.partial(rs_step, 1),
        6: owner_step,
        7: functools.partial(ag_next, gemb, 1, 0),
    }

    def finish_centers(i, slot):
        r = pl.ds(pl.multiple_of(i * JC, JC), JC)
        gu = gt[slot]
        cf = cen[r, :].astype(f32)
        inv = lax.rsqrt(jnp.sum(cf * cf, axis=1, keepdims=True) + epsilon)
        along = jnp.sum(gu * cf, axis=1, keepdims=True) * (inv * inv * inv)
        clow[r, :] = (gu * inv - cf * along).astype(bf16)

    @pl.loop(0, CLASSES // JC)
    def _(i):
        j0 = pl.multiple_of(i * JC, JC)
        r = pl.ds(j0, JC)
        gu = jnp.zeros((JC, D), f32)
        for bt in range(4):
            lab = labels[bt : bt + 1, :] - offset - j0
            hot = lab == lax.broadcasted_iota(jnp.int32, (JC, BT), 0)
            scaled = E[bt, r, :].astype(f32) * rows[bt, 0:1, :]
            gc = jnp.where(hot, rows[bt, 1:2, :], scaled).astype(bf16)
            gu = gu + plain_dot(gc, block(emb, bt))
        gt[lax.rem(i, 2)] = gu
        before = jnp.maximum(i - 1, 0)
        finish_centers(before, lax.rem(i + 1, 2))

        @pl.when(i > 0)
        def _():
            out_copy(before).start()

        for at, step in steps.items():
            @pl.when(i == at)
            def _():
                step()

    finish_centers(CLASSES // JC - 1, (CLASSES // JC - 1) % 2)
    out_copy(CLASSES // JC - 1).start()

    ag_next(gemb, 1, 1)

    others = cols.at[pl.ds(0, N // 2 - 1)]
    pltpu.make_async_copy(others, others, a_send).wait()
    pltpu.make_async_copy(others, others, a_recv).wait()

    start = chip * 2 * F_DEV - tile_of(chip) * 128
    r = lax.broadcasted_iota(jnp.int32, (208, 384), 0)
    want = start + jnp.where(r < 104, core * F_DEV + r, (1 - core) * F_DEV + r - 104)
    pick = (lax.broadcasted_iota(jnp.int32, (208, 384), 1) == want).astype(f32).astype(bf16)
    for h in range(2):
        cols_t[h] = last_dims(pick, cols[h * 32 : (h + 1) * 32].reshape(BT, 384)).astype(bf16)

    ag_next(gemb, 1, 2)
    fc = jnp.zeros((208, D), f32)
    for h in range(2):
        rows_h = jnp.concatenate([gemb[p, core, 2 * h : 2 * h + 2].reshape(BT, 128) for p in range(4)], axis=1)
        fc = fc + plain_dot(cols_t[h], rows_h)
    fc_send[...] = fc[104:208]
    fc_copy = pltpu.make_async_remote_copy(
        src_ref=fc_send, dst_ref=fc_recv, send_sem=d_send.at[1, 0], recv_sem=d_recv.at[1, 0],
        device_id=peer(3, 1), device_id_type=MESH,
    )
    fc_copy.start()
    fc_copy.wait()
    fc_out[...] = (fc[0:104] + fc_recv[...])[0:F_DEV]

    for i in range(CLASSES // JC):
        out_copy(i).wait()
    ag_drain(emb, 0)
    ag_drain(gemb, 1)
    for s in range(3):
        for p in range(4):
            for k in (1, 2, 3):
                rs_copy(s, p, k, ORDERS[p]).wait_send()


def emit_kernel(loss_all, fc, gc_hbm, loss_out, fc_out, out_hbm, held, in_sem, out_sem):
    step = CLASSES // 8

    def read(i):
        r = pl.ds(i * step, step)
        return pltpu.make_async_copy(gc_hbm.at[r], held.at[r], in_sem.at[i])

    def write(i):
        r = pl.ds(i * step, step)
        return pltpu.make_async_copy(held.at[r], out_hbm.at[r], out_sem.at[i])

    for i in range(8):
        read(i).start()
    chip = (lax.axis_index("cls_0") * 4 + lax.axis_index("cls_1")) * 4 + lax.axis_index("cls_2")
    position = lax.axis_index("cls_3") * 64 + chip
    line = loss_all[pl.ds(position // 32, 1), :]
    loss_out[...] = pltpu.roll(line, lax.rem(BT - lax.rem(position, 32) * OWN, BT), 1)[:, 0:OWN]
    fc_out[...] = fc[...]
    for i in range(8):
        read(i).wait()
        write(i).start()
    for i in range(8):
        write(i).wait()


def on_device(features, fc_weight, centers, labels):
    vmem = pl.BlockSpec(memory_space=pltpu.VMEM)
    anywhere = pl.BlockSpec(memory_space=pl.ANY)
    dma = pltpu.SemaphoreType.DMA
    loss_all, grad_fc, grad_centers = pl.pallas_call(
        kernel,
        out_shape=(
            jax.ShapeDtypeStruct((4, BT), f32),
            jax.ShapeDtypeStruct((F_DEV, D), f32),
            jax.ShapeDtypeStruct((CLASSES, D), bf16),
        ),
        in_specs=[vmem, anywhere, anywhere, vmem],
        out_specs=(vmem, vmem, anywhere),
        scratch_shapes=[
            pltpu.VMEM((4, BT), jnp.int32),
            pltpu.VMEM((4, CLASSES, BT), bf16),
            pltpu.VMEM((CLASSES, D), bf16),
            pltpu.VMEM((CLASSES, D), bf16),
            pltpu.VMEM((D, CLASSES), bf16),
            pltpu.VMEM((4, D, BT), bf16),
            pltpu.VMEM((2, D, BT), bf16),
            pltpu.VMEM((4, 2, 4, 4, 4, OWN, 128), bf16),
            pltpu.VMEM((4, 2, 4, 4, 4, OWN, 128), bf16),
            pltpu.VMEM((4, D, BT), f32),
            pltpu.VMEM((2, D, BT), bf16),
            pltpu.VMEM((2, D, BT), bf16),
            pltpu.VMEM((4, 4, 4, 4, OWN, 128), bf16),
            pltpu.VMEM((4, 3, 4, 4, OWN, 128), bf16),
            pltpu.VMEM((4, 4, 4, OWN, 128), bf16),
            pltpu.VMEM((4, 3, 4, OWN, 128), bf16),
            pltpu.VMEM((4, 4, OWN, 128), bf16),
            pltpu.VMEM((4, 3, OWN, 128), bf16),
            pltpu.VMEM((OWN, D), f32),
            pltpu.VMEM((N // 2, OWN, 384), bf16),
            pltpu.VMEM((2, 208, BT), bf16),
            pltpu.VMEM((104, D), f32),
            pltpu.VMEM((104, D), f32),
            pltpu.VMEM((OWN, D), f32),
            pltpu.VMEM((4, 8, BT), f32),
            pltpu.VMEM((3, 7, 8, BT), f32),
            pltpu.VMEM((4, 8, BT), f32),
            dma((N_W,)),
            dma,
            dma((CLASSES // JC,)),
            dma((2, 4, 3, 3)),
            dma((2, 4, 3, 3)),
            dma((3, 4)),
            dma((3, 4)),
            dma((3, 4, 3)),
            dma((3, 4, 3)),
            dma((3, 7)),
            dma((3, 7)),
            dma,
            dma,
        ],
        compiler_params=pltpu.CompilerParams(
            collective_id=0, has_side_effects=True, vmem_limit_bytes=66_000_000
        ),
    )(features, fc_weight, centers, labels.reshape(16, 128))
    loss, grad_fc, grad_centers = pl.pallas_call(
        emit_kernel,
        out_shape=(
            jax.ShapeDtypeStruct((1, OWN), f32),
            jax.ShapeDtypeStruct((F_DEV, D), f32),
            jax.ShapeDtypeStruct((CLASSES, D), bf16),
        ),
        in_specs=[vmem, vmem, anywhere],
        out_specs=(vmem, vmem, anywhere),
        scratch_shapes=[pltpu.VMEM((CLASSES, D), bf16), dma((8,)), dma((8,))],
    )(loss_all, grad_fc, grad_centers)
    return (loss.reshape(-1), grad_centers, grad_fc)


def solution(mesh):
    torus = Mesh(mesh.devices.reshape(4, 4, 4, 2), CLS)
    placed = (P(CLS, None), P(), P(CLS, None), P())
    return jax.shard_map(
        on_device,
        mesh=torus,
        in_specs=placed,
        out_specs=(P(CLS), P(CLS, None), P(CLS, None)),
        check_vma=False,
    )
```

```python
import functools
import math

import jax
import jax.numpy as jnp
from jax import lax
from jax.experimental import pallas as pl
from jax.experimental.pallas import tpu as pltpu
from jax.sharding import Mesh
from jax.sharding import PartitionSpec as P

CLS = ("cls_0", "cls_1", "cls_2", "cls_3")
MESH = pl.DeviceIdType.MESH

logit_scale = 64.0
cos_margin = math.cos(0.5)
sin_margin = math.sin(0.5)
epsilon = 1e-06
exp2_scale = logit_scale / math.log(2.0)

N = 128
D = 512
F = 12544
F_DEV = F // N
OWN = 16
CLASSES = 4096
BT = 512
W_CHUNK = 1792
N_W = F // W_CHUNK
JA = 1024
JB = 2048
JC = 512

ORDERS = ((0, 1, 2), (1, 2, 0), (2, 0, 1), (0, 2, 1), (0, 1, 2))

f32 = jnp.float32
bf16 = jnp.bfloat16


def last_dims(a, b):
    return lax.dot_general(a, b, (((1,), (1,)), ((), ())), preferred_element_type=f32)


def plain_dot(a, b):
    return lax.dot_general(a, b, (((1,), (0,)), ((), ())), preferred_element_type=f32)


def transposed(x):
    width = x.shape[1]
    one = eye(256)
    return jnp.concatenate([last_dims(one, x[:, c : c + 256]) for c in range(0, width, 256)], axis=0).astype(bf16)


def eye(n):
    r = lax.broadcasted_iota(jnp.int32, (n, n), 0)
    c = lax.broadcasted_iota(jnp.int32, (n, n), 1)
    return (r == c).astype(f32).astype(bf16)


def kernel(
    feat_hbm, w_hbm, centers_hbm, labels_hbm,
    loss_out, fc_out, gc_out,
    feat, labels_in, labels, losses,
    E, cen, clow, ct, tt, ttr, emb, emb_t, gemb, gt, gsend, grecv, gs, rb1, gs2, rb2, gs3, rb3, rs_out, cols,
    cols_t, fc_send, fc_recv, own_emb, ar_send, ar_recv, rows,
    w_sem, c_sem, ag_send, ag_recv, d_send, d_recv, rs_send, rs_recv,
    s_send, s_recv, a_send, a_recv,
):
    me = tuple(lax.axis_index(name) for name in CLS)
    core = me[3]
    idx = ((me[0] * 4 + me[1]) * 4 + me[2]) * 2 + core
    offset = idx * CLASSES
    chip = idx // 2

    def peer(axis, k):
        size = 2 if axis == 3 else 4
        coords = list(me)
        coords[axis] = lax.rem(me[axis] + k, size)
        return tuple(coords)

    def w_copy(i):
        return pltpu.make_async_copy(
            w_hbm.at[pl.ds(i * W_CHUNK, W_CHUNK)],
            E.at[i // 2, pl.ds((i % 2) * 2048, W_CHUNK)],
            w_sem.at[i],
        )

    feat_fetch = pltpu.make_async_copy(feat_hbm, feat, c_sem.at[1])
    labels_fetch = pltpu.make_async_copy(labels_hbm, labels_in, c_sem.at[2])
    c_copy = pltpu.make_async_copy(centers_hbm, cen, c_sem.at[0])
    feat_fetch.start()
    labels_fetch.start()
    for i in range(N_W):
        w_copy(i).start()
    c_copy.start()

    barrier = pltpu.get_barrier_semaphore()
    for axis in range(3):
        for k in (2, 1, 3):
            pl.semaphore_signal(barrier, inc=1, device_id=peer(axis, k), device_id_type=MESH)
    pl.semaphore_signal(barrier, inc=1, device_id=peer(3, 1), device_id_type=MESH)

    labels_fetch.wait()
    lane = lax.broadcasted_iota(jnp.int32, (16, 128), 1)
    for c in range(2):
        low = labels_in[...]
        for m in range(4):
            moved = pltpu.roll(labels_in[...], (-16 * m - 16 * c) % 128, 1)
            low = jnp.where(lane // 16 == m, moved, low)
        high = pltpu.roll(low, 64, 1)
        for g in range(8):
            line = jnp.where(lane[0:1] < 64, low[2 * g : 2 * g + 1], high[2 * g + 1 : 2 * g + 2])
            labels[2 * c + g // 4 : 2 * c + g // 4 + 1, (g % 4) * 128 : (g % 4 + 1) * 128] = line

    feat_fetch.wait()
    acc = jnp.zeros((OWN, D), f32)
    for i in range(N_W):
        w_copy(i).wait()
        at = (i % 2) * 2048
        acc = acc + plain_dot(feat[:, i * W_CHUNK : (i + 1) * W_CHUNK], E[i // 2, at : at + W_CHUNK])
    own = acc.astype(bf16).astype(f32)
    own_inv = lax.rsqrt(jnp.sum(own * own, axis=1, keepdims=True) + epsilon)
    own_emb[...] = own
    own_low = (own * own_inv).astype(bf16)

    def put_own(buf, value):
        for p in range(4):
            buf[p, core, me[0], me[1], me[2]] = value[:, p * 128 : (p + 1) * 128]

    def view(buf, p, gathered, at=None):
        at = me if at is None else at
        where = tuple(slice(None) if a in gathered else at[a] for a in range(3))
        return buf.at[(p, core) + where]

    def by_order(p, act):
        if p < 3:
            act(ORDERS[p])
            return
        for c in range(2):
            @pl.when(core == c)
            def _():
                act(ORDERS[3 + c])

    def ag_copy(buf, inst, p, s, k, order):
        v = view(buf, p, order[:s])
        return pltpu.make_async_remote_copy(
            src_ref=v, dst_ref=v,
            send_sem=ag_send.at[inst, p, s, k - 1], recv_sem=ag_recv.at[inst, p, s, k - 1],
            device_id=peer(order[s], k), device_id_type=MESH,
        )

    def ag_start(buf, inst, p, s):
        def act(order):
            for k in (2, 1, 3):
                ag_copy(buf, inst, p, s, k, order).start()

        by_order(p, act)

    def ag_next(buf, inst, s):
        for p in range(4):
            for k in (2, 1, 3):
                ag_copy(buf, inst, p, s, k, ORDERS[p]).wait_recv()
            if s < 2:
                ag_start(buf, inst, p, s + 1)
            elif inst == 0:
                pair_copy(buf, inst, p).start()

    def ag_drain(buf, inst):
        for s in range(3):
            for k in (2, 1, 3):
                for p in range(4):
                    ag_copy(buf, inst, p, s, k, ORDERS[p]).wait_send()

    def pair_copy(buf, inst, p):
        v = buf.at[p, core]
        return pltpu.make_async_remote_copy(
            src_ref=v, dst_ref=v,
            send_sem=d_send.at[inst, p], recv_sem=d_recv.at[inst, p],
            device_id=peer(3, 1), device_id_type=MESH,
        )

    def pair_wait(buf, inst):
        for p in range(4):
            pair_copy(buf, inst, p).wait()

    def block(buf, bt):
        c, y0 = bt // 2, (bt % 2) * 2
        return jnp.concatenate([buf[p, c, pl.ds(y0, 2)].reshape(BT, 128) for p in range(4)], axis=1)

    put_own(emb, own_low)
    pl.semaphore_wait(barrier, 10)
    for p in range(4):
        ag_start(emb, 0, p, 0)

    c_copy.wait()

    @pl.loop(0, CLASSES // JC)
    def _(i):
        r = pl.ds(pl.multiple_of(i * JC, JC), JC)
        cf = cen[r, :].astype(f32)
        inv = lax.rsqrt(jnp.sum(cf * cf, axis=1, keepdims=True) + epsilon)
        low = (cf * inv).astype(bf16)
        clow[r, :] = low
        ct[:, r] = transposed(low)

        @pl.when(i == 4)
        def _():
            ag_next(emb, 0, 0)

    @pl.loop(0, 4)
    def _(bt):
        lab = labels[pl.ds(bt, 1), :] - offset
        total = jnp.zeros((D, BT), f32)
        for j0 in range(0, CLASSES, JB):
            hot = (lab - j0) == lax.broadcasted_iota(jnp.int32, (JB, BT), 0)
            hot = jnp.where(hot, 1.0, 0.0).astype(bf16)
            total = total + plain_dot(ct[:, j0 : j0 + JB], hot)
        tt[bt] = total.astype(bf16)

        @pl.when(bt == 0)
        def _():
            ag_next(emb, 0, 1)

    ag_next(emb, 0, 2)

    def tt_copy():
        return pltpu.make_async_remote_copy(
            src_ref=tt.at[pl.ds(2 * (1 - core), 2)], dst_ref=ttr,
            send_sem=d_send.at[1, 1], recv_sem=d_recv.at[1, 1], device_id=peer(3, 1), device_id_type=MESH,
        )

    tt_copy().start()
    def tile_of(c):
        return jnp.minimum((c * 2 * F_DEV) // 128, F // 128 - 3)

    def feature_copy(k):
        to = lax.bitwise_and(chip + k, N // 2 - 1)
        coords = (
            lax.shift_right_logical(to, 4), lax.bitwise_and(lax.shift_right_logical(to, 2), 3), lax.bitwise_and(to, 3), core
        )
        return pltpu.make_async_remote_copy(
            src_ref=feat.at[:, pl.ds(pl.multiple_of(tile_of(to) * 128, 128), 384)],
            dst_ref=cols.at[chip],
            send_sem=a_send, recv_sem=a_recv, device_id=coords, device_id_type=MESH,
        )

    cols[chip] = feat[:, pl.ds(pl.multiple_of(tile_of(chip) * 128, 128), 384)]

    rows[...] = jnp.zeros_like(rows)
    n_a = CLASSES // JA

    def side(n):
        return lax.rem(n + 2 * core, 4)

    def turn(n):
        emb_t[side(n)] = transposed(block(emb, side(n)))

    def cosine_tile(n, a):
        slot = 2 * (a % 2)
        gt[slot : slot + 2] = plain_dot(clow[a * JA : (a + 1) * JA, :], emb_t[side(n)]).reshape(2, BT, BT)

    def exp_tile(n, a):
        slot = 2 * (a % 2)
        cosines = gt[slot : slot + 2].reshape(JA, BT)
        lab = labels[pl.ds(side(n), 1), :] - offset - a * JA
        hot = lab == lax.broadcasted_iota(jnp.int32, (JA, BT), 0)
        e = jnp.where(hot, 0.0, jnp.exp2(cosines * exp2_scale))
        rows[side(n)] += jnp.sum(e.reshape(JA // 8, 8, BT), axis=0)
        E[side(n), a * JA : (a + 1) * JA, :] = e.astype(bf16)

    turn(0)
    turn(1)
    cosine_tile(0, 0)

    @pl.loop(0, 3)
    def _(n):
        @pl.when(n == 1)
        def _():
            pair_wait(emb, 0)
            turn(2)
            turn(3)

        for u in range(21):
            feature_copy(n * 21 + u + 1).start()
        for a in range(n_a):
            if a + 1 < n_a:
                cosine_tile(n, a + 1)
            else:
                cosine_tile(n + 1, 0)
            exp_tile(n, a)

    for a in range(n_a):
        if a + 1 < n_a:
            cosine_tile(3, a + 1)
        exp_tile(3, a)

    def margin(tc):
        ts = jnp.sqrt(1.0 - tc * tc)
        margined = logit_scale * (tc * cos_margin - ts * sin_margin)
        return margined, cos_margin + sin_margin * tc / ts

    def on_chip(bt):
        lab = labels[pl.ds(bt, 1), :] - chip * (2 * CLASSES)
        return jnp.logical_and(lab >= 0, lab < 2 * CLASSES)

    ar_send[0, 4:8, :] = jnp.zeros((4, BT), f32)
    for bt in range(4):
        ar_send[0, bt : bt + 1, :] = jnp.sum(rows[bt], axis=0, keepdims=True)
    tt_copy().wait()
    for h in range(2):
        bt = 2 * core + h
        rows_t = tt[bt].astype(f32) + ttr[h].astype(f32)
        ttr[h] = rows_t.astype(bf16)
        tc = jnp.sum(emb_t[bt].astype(f32) * rows_t, axis=0, keepdims=True)
        margined, _ = margin(tc)
        ar_send[0, pl.ds(bt, 1), :] += jnp.where(on_chip(bt), jnp.exp(margined), 0.0)
        ar_send[0, pl.ds(4 + bt, 1), :] = tc

    AR_PEERS = (
        tuple((z, c) for z in (2, 1, 3, 0) for c in range(2) if z + c > 0),
        tuple((1, k) for k in (2, 1, 3)),
        tuple((0, k) for k in (2, 1, 3)),
    )

    def ar_copy(s, n):
        if s == 0:
            dz, dc = AR_PEERS[0][n]
            to = (me[0], me[1], lax.rem(me[2] + dz, 4), lax.rem(core + dc, 2))
        else:
            to = peer(*AR_PEERS[s][n])
        return pltpu.make_async_remote_copy(
            src_ref=ar_send.at[s], dst_ref=ar_recv.at[s, n],
            send_sem=s_send.at[s, n], recv_sem=s_recv.at[s, n],
            device_id=to, device_id_type=MESH,
        )

    def ar_start(s):
        for n in range(len(AR_PEERS[s])):
            ar_copy(s, n).start()

    def ar_finish(s):
        total = ar_send[s]
        for n in range(len(AR_PEERS[s])):
            ar_copy(s, n).wait_recv()
            total = total + ar_recv[s, n]
        ar_send[s + 1] = total
        if s < 2:
            ar_start(s + 1)

    ar_start(0)

    def g_copy(h):
        return pltpu.make_async_remote_copy(
            src_ref=gsend.at[h], dst_ref=grecv.at[h],
            send_sem=d_send.at[2, h], recv_sem=d_recv.at[2, h], device_id=peer(3, 1), device_id_type=MESH,
        )

    half = CLASSES // 2

    @pl.loop(0, 4)
    def _(i):
        bt = lax.rem(i + 2 * core + 2, 4)
        gt[i] = plain_dot(ct[:, 0:half], E[bt, 0:half, :])

        @pl.when(i == 1)
        def _():
            ar_finish(0)

        gt[i] += plain_dot(ct[:, half:], E[bt, half:, :])

        @pl.when(i == 2)
        def _():
            ar_finish(1)

        @pl.when(i < 2)
        def _():
            gsend[i] = gt[i].astype(bf16)
            g_copy(i).start()

    ar_finish(2)
    for s in range(3):
        for n in range(len(AR_PEERS[s])):
            ar_copy(s, n).wait_send()

    for bt in range(4):
        total = ar_send[3, bt : bt + 1, :]
        margined, slope = margin(ar_send[3, 4 + bt : 5 + bt, :])
        losses[bt : bt + 1, :] = jnp.log(total) - margined
        scale = logit_scale / total
        rows[bt, 0:1, :] = scale
        rows[bt, 1:2, :] = (jnp.exp(margined) - total) * slope * scale

    for h in range(2):
        bt = 2 * core + h
        g_copy(h).wait()
        v = jnp.where(on_chip(bt), rows[bt, 1:2, :], 0.0)
        g = (gt[2 + h] + grecv[h].astype(f32)) * rows[bt, 0:1, :] + v * ttr[h].astype(f32)
        back = transposed(g.astype(bf16))
        for p in range(4):
            gs[p, 2 * h : 2 * h + 2] = back[:, p * 128 : (p + 1) * 128].reshape(2, 4, 4, OWN, 128)

    def rs_copy(s, p, k, order):
        axis = order[2 - s]
        to = peer(axis, k)
        if s == 0:
            src = gs.at[(p,) + tuple(to[a] if a == axis else slice(None) for a in range(3))]
            dst = rb1.at[p, k - 1]
        elif s == 1:
            left = sorted(order[:2])
            src = gs2.at[(p,) + tuple(to[a] if a == axis else slice(None) for a in left)]
            dst = rb2.at[p, k - 1]
        else:
            src = gs3.at[p, to[axis]]
            dst = rb3.at[p, k - 1]
        return pltpu.make_async_remote_copy(
            src_ref=src, dst_ref=dst,
            send_sem=rs_send.at[s, p, k - 1], recv_sem=rs_recv.at[s, p, k - 1],
            device_id=to, device_id_type=MESH,
        )

    def rs_start(s, p):
        def act(order):
            for k in (2, 1, 3):
                rs_copy(s, p, k, order).start()

        by_order(p, act)

    def rs_step(s):
        bufs = (rb1, rb2, rb3)[s]
        for p in range(4):
            for k in (2, 1, 3):
                rs_copy(s, p, k, ORDERS[p]).wait_recv()

            def act(order):
                axis = order[2 - s]
                if s == 0:
                    total = gs[(p,) + tuple(me[a] if a == axis else slice(None) for a in range(3))]
                elif s == 1:
                    total = gs2[(p,) + tuple(me[a] if a == axis else slice(None) for a in sorted(order[:2]))]
                else:
                    total = gs3[p, me[axis]]
                total = total.astype(f32)
                for k in (2, 1, 3):
                    total = total + bufs[p, k - 1].astype(f32)
                if s == 0:
                    gs2[p] = total.astype(bf16)
                elif s == 1:
                    gs3[p] = total.astype(bf16)
                else:
                    rs_out[:, p * 128 : (p + 1) * 128] = total
                if s < 2:
                    for k in (2, 1, 3):
                        rs_copy(s + 1, p, k, order).start()

            by_order(p, act)

    def owner_step():
        rs_step(2)
        grad_dir = rs_out[...]
        own = own_emb[...]
        inv = lax.rsqrt(jnp.sum(own * own, axis=1, keepdims=True) + epsilon)
        direction = own * inv
        along = jnp.sum(grad_dir * direction, axis=1, keepdims=True)
        put_own(gemb, ((grad_dir - direction * along) * inv).astype(bf16))
        for p in range(4):
            ag_start(gemb, 1, p, 0)

    for p in range(4):
        rs_start(0, p)

    steps = {
        2: functools.partial(rs_step, 0),
        4: functools.partial(rs_step, 1),
        5: owner_step,
        7: functools.partial(ag_next, gemb, 1, 0),
    }

    def finish_centers(i, slot):
        r = pl.ds(pl.multiple_of(i * JC, JC), JC)
        gu = gt[slot]
        cf = cen[r, :].astype(f32)
        inv = lax.rsqrt(jnp.sum(cf * cf, axis=1, keepdims=True) + epsilon)
        along = jnp.sum(gu * cf, axis=1, keepdims=True) * (inv * inv * inv)
        gc_out[r, :] = (gu * inv - cf * along).astype(bf16)

    @pl.loop(0, CLASSES // JC)
    def _(i):
        j0 = pl.multiple_of(i * JC, JC)
        r = pl.ds(j0, JC)
        gu = jnp.zeros((JC, D), f32)
        for bt in range(4):
            lab = labels[bt : bt + 1, :] - offset - j0
            hot = lab == lax.broadcasted_iota(jnp.int32, (JC, BT), 0)
            scaled = E[bt, r, :].astype(f32) * rows[bt, 0:1, :]
            gc = jnp.where(hot, rows[bt, 1:2, :], scaled).astype(bf16)
            gu = gu + plain_dot(gc, block(emb, bt))
        gt[lax.rem(i, 2)] = gu
        before = jnp.maximum(i - 1, 0)
        finish_centers(before, lax.rem(i + 1, 2))

        for at, step in steps.items():
            @pl.when(i == at)
            def _():
                step()

    finish_centers(CLASSES // JC - 1, (CLASSES // JC - 1) % 2)
    position = core * (N // 2) + chip
    line = jnp.zeros((1, BT), f32)
    for bt in range(4):
        line = jnp.where(position // 32 == bt, losses[bt : bt + 1, :], line)
    line = jnp.broadcast_to(line, (8, BT))
    for bit in (1, 2, 4, 8, 16):
        moved = pltpu.roll(line, BT - bit * OWN, 1)
        line = jnp.where(lax.rem(position // bit, 2) == 1, moved, line)
    loss_out[...] = line[:, 0:128]

    ag_next(gemb, 1, 1)

    others = cols.at[pl.ds(0, N // 2 - 1)]
    pltpu.make_async_copy(others, others, a_send).wait()
    pltpu.make_async_copy(others, others, a_recv).wait()

    start = chip * 2 * F_DEV - tile_of(chip) * 128
    r = lax.broadcasted_iota(jnp.int32, (208, 384), 0)
    want = start + jnp.where(r < 104, core * F_DEV + r, (1 - core) * F_DEV + r - 104)
    pick = (lax.broadcasted_iota(jnp.int32, (208, 384), 1) == want).astype(f32).astype(bf16)
    for h in range(2):
        cols_t[h] = last_dims(pick, cols[h * 32 : (h + 1) * 32].reshape(BT, 384)).astype(bf16)

    ag_next(gemb, 1, 2)
    fc = jnp.zeros((208, D), f32)
    for h in range(2):
        rows_h = jnp.concatenate([gemb[p, core, 2 * h : 2 * h + 2].reshape(BT, 128) for p in range(4)], axis=1)
        fc = fc + plain_dot(cols_t[h], rows_h)
    fc_send[...] = fc[104:208]
    fc_copy = pltpu.make_async_remote_copy(
        src_ref=fc_send, dst_ref=fc_recv, send_sem=d_send.at[1, 0], recv_sem=d_recv.at[1, 0],
        device_id=peer(3, 1), device_id_type=MESH,
    )
    fc_copy.start()
    fc_copy.wait()
    fc_out[...] = fc[0:104] + fc_recv[...]

    ag_drain(emb, 0)
    ag_drain(gemb, 1)
    for s in range(3):
        for p in range(4):
            for k in (2, 1, 3):
                rs_copy(s, p, k, ORDERS[p]).wait_send()


def on_device(features, fc_weight, centers, labels):
    vmem = pl.BlockSpec(memory_space=pltpu.VMEM)
    anywhere = pl.BlockSpec(memory_space=pl.ANY)
    dma = pltpu.SemaphoreType.DMA
    loss, grad_fc, grad_centers = pl.pallas_call(
        kernel,
        out_shape=(
            pltpu.VMEM((8, 128), f32),
            pltpu.VMEM((104, D), f32),
            pltpu.VMEM((CLASSES, D), bf16),
        ),
        in_specs=[anywhere] * 4,
        out_specs=(vmem, vmem, vmem),
        scratch_shapes=[
            pltpu.VMEM((OWN, F), bf16),
            pltpu.VMEM((16, 128), jnp.int32),
            pltpu.VMEM((4, BT), jnp.int32),
            pltpu.VMEM((8, BT), f32),
            pltpu.VMEM((4, CLASSES, BT), bf16),
            pltpu.VMEM((CLASSES, D), bf16),
            pltpu.VMEM((CLASSES, D), bf16),
            pltpu.VMEM((D, CLASSES), bf16),
            pltpu.VMEM((4, D, BT), bf16),
            pltpu.VMEM((2, D, BT), bf16),
            pltpu.VMEM((4, 2, 4, 4, 4, OWN, 128), bf16),
            pltpu.VMEM((4, D, BT), bf16),
            pltpu.VMEM((4, 2, 4, 4, 4, OWN, 128), bf16),
            pltpu.VMEM((4, D, BT), f32),
            pltpu.VMEM((2, D, BT), bf16),
            pltpu.VMEM((2, D, BT), bf16),
            pltpu.VMEM((4, 4, 4, 4, OWN, 128), bf16),
            pltpu.VMEM((4, 3, 4, 4, OWN, 128), bf16),
            pltpu.VMEM((4, 4, 4, OWN, 128), bf16),
            pltpu.VMEM((4, 3, 4, OWN, 128), bf16),
            pltpu.VMEM((4, 4, OWN, 128), bf16),
            pltpu.VMEM((4, 3, OWN, 128), bf16),
            pltpu.VMEM((OWN, D), f32),
            pltpu.VMEM((N // 2, OWN, 384), bf16),
            pltpu.VMEM((2, 208, BT), bf16),
            pltpu.VMEM((104, D), f32),
            pltpu.VMEM((104, D), f32),
            pltpu.VMEM((OWN, D), f32),
            pltpu.VMEM((4, 8, BT), f32),
            pltpu.VMEM((3, 7, 8, BT), f32),
            pltpu.VMEM((4, 8, BT), f32),
            dma((N_W,)),
            dma((3,)),
            dma((2, 4, 3, 3)),
            dma((2, 4, 3, 3)),
            dma((3, 4)),
            dma((3, 4)),
            dma((3, 4, 3)),
            dma((3, 4, 3)),
            dma((3, 7)),
            dma((3, 7)),
            dma,
            dma,
        ],
        compiler_params=pltpu.CompilerParams(
            collective_id=0, has_side_effects=True, vmem_limit_bytes=58_000_000
        ),
    )(features, fc_weight, centers, labels.reshape(16, 128))
    return (loss[0, :OWN], grad_centers, grad_fc[:F_DEV])


def solution(mesh):
    torus = Mesh(mesh.devices.reshape(4, 4, 4, 2), CLS)
    placed = (P(CLS, None), P(), P(CLS, None), P())
    return jax.shard_map(
        on_device,
        mesh=torus,
        in_specs=placed,
        out_specs=(P(CLS), P(CLS, None), P(CLS, None)),
        check_vma=False,
    )
```

```python
import functools
import math

import jax
import jax.numpy as jnp
from jax import lax
from jax.experimental import pallas as pl
from jax.experimental.pallas import tpu as pltpu
from jax.sharding import Mesh
from jax.sharding import PartitionSpec as P

CLS = ("cls_0", "cls_1", "cls_2", "cls_3")
MESH = pl.DeviceIdType.MESH

logit_scale = 64.0
cos_margin = math.cos(0.5)
sin_margin = math.sin(0.5)
epsilon = 1e-06
exp2_scale = logit_scale / math.log(2.0)

N = 128
D = 512
F = 12544
F_DEV = F // N
OWN = 16
CLASSES = 4096
BT = 512
W_CHUNK = 1792
N_W = F // W_CHUNK
JA = 1024
JB = 2048
JC = 512

ORDERS = ((0, 1, 2), (1, 2, 0), (2, 0, 1), (0, 2, 1), (0, 1, 2))

f32 = jnp.float32
bf16 = jnp.bfloat16


def last_dims(a, b):
    return lax.dot_general(a, b, (((1,), (1,)), ((), ())), preferred_element_type=f32)


def plain_dot(a, b):
    return lax.dot_general(a, b, (((1,), (0,)), ((), ())), preferred_element_type=f32)


def transposed(x):
    width = x.shape[1]
    one = eye(256)
    return jnp.concatenate([last_dims(one, x[:, c : c + 256]) for c in range(0, width, 256)], axis=0).astype(bf16)


def eye(n):
    r = lax.broadcasted_iota(jnp.int32, (n, n), 0)
    c = lax.broadcasted_iota(jnp.int32, (n, n), 1)
    return (r == c).astype(f32).astype(bf16)


def kernel(
    feat_hbm, w_hbm, centers_hbm, labels_hbm,
    loss_out, fc_out, gc_out,
    feat, labels_in, labels, losses,
    E, cen, clow, ct, tt, ttr, emb, emb_t, gemb, gt, gsend, grecv, gs, rb1, gs2, rb2, gs3, rb3, cols,
    cols_t, fc_send, fc_recv, ar_send, ar_recv, rows,
    w_sem, c_sem, ag_send, ag_recv, d_send, d_recv, rs_send, rs_recv,
    s_send, s_recv, a_send, a_recv,
):
    me = tuple(lax.axis_index(name) for name in CLS)
    core = me[3]
    idx = ((me[0] * 4 + me[1]) * 4 + me[2]) * 2 + core
    offset = idx * CLASSES
    chip = idx // 2

    def peer(axis, k):
        size = 2 if axis == 3 else 4
        coords = list(me)
        coords[axis] = lax.rem(me[axis] + k, size)
        return tuple(coords)

    def w_copy(i):
        return pltpu.make_async_copy(
            w_hbm.at[pl.ds(i * W_CHUNK, W_CHUNK)],
            E.at[i // 2, pl.ds((i % 2) * 2048, W_CHUNK)],
            w_sem.at[i],
        )

    feat_fetch = pltpu.make_async_copy(feat_hbm, feat, c_sem.at[1])
    labels_fetch = pltpu.make_async_copy(labels_hbm, labels_in, c_sem.at[2])
    c_copy = pltpu.make_async_copy(centers_hbm, cen, c_sem.at[0])
    feat_fetch.start()
    labels_fetch.start()
    for i in range(N_W):
        w_copy(i).start()
    c_copy.start()

    barrier = pltpu.get_barrier_semaphore()
    for axis in range(3):
        for k in (2, 1, 3):
            pl.semaphore_signal(barrier, inc=1, device_id=peer(axis, k), device_id_type=MESH)
    pl.semaphore_signal(barrier, inc=1, device_id=peer(3, 1), device_id_type=MESH)

    labels_fetch.wait()
    lane = lax.broadcasted_iota(jnp.int32, (16, 128), 1)
    for c in range(2):
        low = labels_in[...]
        for m in range(4):
            moved = pltpu.roll(labels_in[...], (-16 * m - 16 * c) % 128, 1)
            low = jnp.where(lane // 16 == m, moved, low)
        high = pltpu.roll(low, 64, 1)
        for g in range(8):
            line = jnp.where(lane[0:1] < 64, low[2 * g : 2 * g + 1], high[2 * g + 1 : 2 * g + 2])
            labels[2 * c + g // 4 : 2 * c + g // 4 + 1, (g % 4) * 128 : (g % 4 + 1) * 128] = line

    feat_fetch.wait()
    acc = jnp.zeros((OWN, D), f32)
    for i in range(N_W):
        w_copy(i).wait()
        at = (i % 2) * 2048
        acc = acc + plain_dot(feat[:, i * W_CHUNK : (i + 1) * W_CHUNK], E[i // 2, at : at + W_CHUNK])
    own = acc.astype(bf16).astype(f32)
    own_inv = lax.rsqrt(jnp.sum(own * own, axis=1, keepdims=True) + epsilon)
    own_low = (own * own_inv).astype(bf16)

    def put_own(buf, value):
        for p in range(4):
            buf[p, core, me[0], me[1], me[2]] = value[:, p * 128 : (p + 1) * 128]

    def view(buf, p, gathered, at=None):
        at = me if at is None else at
        where = tuple(slice(None) if a in gathered else at[a] for a in range(3))
        return buf.at[(p, core) + where]

    def by_order(p, act):
        if p < 3:
            act(ORDERS[p])
            return
        for c in range(2):
            @pl.when(core == c)
            def _():
                act(ORDERS[3 + c])

    def ag_copy(buf, inst, p, s, k, order):
        v = view(buf, p, order[:s])
        return pltpu.make_async_remote_copy(
            src_ref=v, dst_ref=v,
            send_sem=ag_send.at[inst, p, s, k - 1], recv_sem=ag_recv.at[inst, p, s, k - 1],
            device_id=peer(order[s], k), device_id_type=MESH,
        )

    def ag_start(buf, inst, p, s):
        def act(order):
            for k in (2, 1, 3):
                ag_copy(buf, inst, p, s, k, order).start()

        by_order(p, act)

    def ag_next(buf, inst, s):
        for p in range(4):
            for k in (2, 1, 3):
                ag_copy(buf, inst, p, s, k, ORDERS[p]).wait_recv()
            if s < 2:
                ag_start(buf, inst, p, s + 1)
            elif inst == 0:
                pair_copy(buf, inst, p).start()

    def ag_drain(buf, inst):
        for s in range(inst, 3):
            for k in (2, 1, 3):
                for p in range(4):
                    ag_copy(buf, inst, p, s, k, ORDERS[p]).wait_send()

    def pair_copy(buf, inst, p):
        v = buf.at[p, core]
        return pltpu.make_async_remote_copy(
            src_ref=v, dst_ref=v,
            send_sem=d_send.at[inst, p], recv_sem=d_recv.at[inst, p],
            device_id=peer(3, 1), device_id_type=MESH,
        )

    def pair_wait(buf, inst):
        for p in range(4):
            pair_copy(buf, inst, p).wait()

    def block(buf, bt):
        c, y0 = bt // 2, (bt % 2) * 2
        return jnp.concatenate([buf[p, c, pl.ds(y0, 2)].reshape(BT, 128) for p in range(4)], axis=1)

    put_own(emb, own_low)
    pl.semaphore_wait(barrier, 10)
    for p in range(4):
        ag_start(emb, 0, p, 0)

    feat[...] = (feat[...].astype(f32) * own_inv).astype(bf16)

    c_copy.wait()

    @pl.loop(0, CLASSES // JC)
    def _(i):
        r = pl.ds(pl.multiple_of(i * JC, JC), JC)
        cf = cen[r, :].astype(f32)
        inv = lax.rsqrt(jnp.sum(cf * cf, axis=1, keepdims=True) + epsilon)
        low = (cf * inv).astype(bf16)
        clow[r, :] = low
        ct[:, r] = transposed(low)

        @pl.when(i == 5)
        def _():
            ag_next(emb, 0, 0)

    @pl.loop(0, 4)
    def _(bt):
        lab = labels[pl.ds(bt, 1), :] - offset
        total = jnp.zeros((D, BT), f32)
        for j0 in range(0, CLASSES, JB):
            hot = (lab - j0) == lax.broadcasted_iota(jnp.int32, (JB, BT), 0)
            hot = jnp.where(hot, 1.0, 0.0).astype(bf16)
            total = total + plain_dot(ct[:, j0 : j0 + JB], hot)
        tt[bt] = total.astype(bf16)

        @pl.when(bt == 0)
        def _():
            ag_next(emb, 0, 1)

    ag_next(emb, 0, 2)

    def tt_copy():
        return pltpu.make_async_remote_copy(
            src_ref=tt.at[pl.ds(2 * (1 - core), 2)], dst_ref=ttr,
            send_sem=d_send.at[1, 1], recv_sem=d_recv.at[1, 1], device_id=peer(3, 1), device_id_type=MESH,
        )

    tt_copy().start()
    def tile_of(c):
        return jnp.minimum((c * 2 * F_DEV) // 128, F // 128 - 3)

    def feature_copy(k):
        to = lax.bitwise_and(chip + k, N // 2 - 1)
        coords = (
            lax.shift_right_logical(to, 4), lax.bitwise_and(lax.shift_right_logical(to, 2), 3), lax.bitwise_and(to, 3), core
        )
        return pltpu.make_async_remote_copy(
            src_ref=feat.at[:, pl.ds(pl.multiple_of(tile_of(to) * 128, 128), 384)],
            dst_ref=cols.at[chip],
            send_sem=a_send, recv_sem=a_recv, device_id=coords, device_id_type=MESH,
        )

    cols[chip] = feat[:, pl.ds(pl.multiple_of(tile_of(chip) * 128, 128), 384)]

    rows[...] = jnp.zeros_like(rows)
    n_a = CLASSES // JA

    def side(n):
        return lax.rem(n + 2 * core, 4)

    def turn(n):
        emb_t[side(n)] = transposed(block(emb, side(n)))

    def cosine_tile(n, a):
        slot = 2 * (a % 2)
        gt[slot : slot + 2] = plain_dot(clow[a * JA : (a + 1) * JA, :], emb_t[side(n)]).reshape(2, BT, BT)

    def exp_tile(n, a):
        slot = 2 * (a % 2)
        cosines = gt[slot : slot + 2].reshape(JA, BT)
        lab = labels[pl.ds(side(n), 1), :] - offset - a * JA
        hot = lab == lax.broadcasted_iota(jnp.int32, (JA, BT), 0)
        e = jnp.where(hot, 0.0, jnp.exp2(cosines * exp2_scale))
        rows[side(n)] += jnp.sum(e.reshape(JA // 8, 8, BT), axis=0)
        E[side(n), a * JA : (a + 1) * JA, :] = e.astype(bf16)

    turn(0)
    turn(1)
    cosine_tile(0, 0)

    @pl.loop(0, 3)
    def _(n):
        @pl.when(n == 1)
        def _():
            pair_wait(emb, 0)
            turn(2)
            turn(3)

        for u in range(21):
            feature_copy(n * 21 + u + 1).start()
        for a in range(n_a):
            if a + 1 < n_a:
                cosine_tile(n, a + 1)
            else:
                cosine_tile(n + 1, 0)
            exp_tile(n, a)

    for a in range(n_a):
        if a + 1 < n_a:
            cosine_tile(3, a + 1)
        exp_tile(3, a)

    def margin(tc):
        ts = jnp.sqrt(1.0 - tc * tc)
        margined = logit_scale * (tc * cos_margin - ts * sin_margin)
        return margined, cos_margin + sin_margin * tc / ts

    def on_chip(bt):
        lab = labels[pl.ds(bt, 1), :] - chip * (2 * CLASSES)
        return jnp.logical_and(lab >= 0, lab < 2 * CLASSES)

    ar_send[0, 4:8, :] = jnp.zeros((4, BT), f32)
    for bt in range(4):
        ar_send[0, bt : bt + 1, :] = jnp.sum(rows[bt], axis=0, keepdims=True)
    tt_copy().wait()
    for h in range(2):
        bt = 2 * core + h
        rows_t = tt[bt].astype(f32) + ttr[h].astype(f32)
        ttr[h] = rows_t.astype(bf16)
        tc = jnp.sum(emb_t[bt].astype(f32) * rows_t, axis=0, keepdims=True)
        margined, _ = margin(tc)
        ar_send[0, pl.ds(bt, 1), :] += jnp.where(on_chip(bt), jnp.exp(margined), 0.0)
        ar_send[0, pl.ds(4 + bt, 1), :] = tc

    AR_PEERS = (
        tuple((z, c) for z in (2, 1, 3, 0) for c in range(2) if z + c > 0),
        tuple((1, k) for k in (2, 1, 3)),
        tuple((0, k) for k in (2, 1, 3)),
    )

    def ar_copy(s, n):
        if s == 0:
            dz, dc = AR_PEERS[0][n]
            to = (me[0], me[1], lax.rem(me[2] + dz, 4), lax.rem(core + dc, 2))
        else:
            to = peer(*AR_PEERS[s][n])
        return pltpu.make_async_remote_copy(
            src_ref=ar_send.at[s], dst_ref=ar_recv.at[s, n],
            send_sem=s_send.at[s, n], recv_sem=s_recv.at[s, n],
            device_id=to, device_id_type=MESH,
        )

    def ar_start(s):
        for n in range(len(AR_PEERS[s])):
            ar_copy(s, n).start()

    def ar_finish(s):
        total = ar_send[s]
        for n in range(len(AR_PEERS[s])):
            ar_copy(s, n).wait_recv()
            total = total + ar_recv[s, n]
        ar_send[s + 1] = total
        if s < 2:
            ar_start(s + 1)

    ar_start(0)

    def g_copy(h):
        return pltpu.make_async_remote_copy(
            src_ref=gsend.at[h], dst_ref=grecv.at[h],
            send_sem=d_send.at[2, h], recv_sem=d_recv.at[2, h], device_id=peer(3, 1), device_id_type=MESH,
        )

    half = CLASSES // 2

    @pl.loop(0, 4)
    def _(i):
        bt = lax.rem(i + 2 * core + 2, 4)
        gt[i] = plain_dot(ct[:, 0:half], E[bt, 0:half, :])

        @pl.when(i == 1)
        def _():
            ar_finish(0)

        gt[i] += plain_dot(ct[:, half:], E[bt, half:, :])

        @pl.when(i == 2)
        def _():
            ar_finish(1)

        @pl.when(i < 2)
        def _():
            gsend[i] = gt[i].astype(bf16)
            g_copy(i).start()

    ar_finish(2)
    for s in range(3):
        for n in range(len(AR_PEERS[s])):
            ar_copy(s, n).wait_send()

    for bt in range(4):
        total = ar_send[3, bt : bt + 1, :]
        margined, slope = margin(ar_send[3, 4 + bt : 5 + bt, :])
        losses[bt : bt + 1, :] = jnp.log(total) - margined
        scale = logit_scale / total
        rows[bt, 0:1, :] = scale
        rows[bt, 1:2, :] = (jnp.exp(margined) - total) * slope * scale

    for h in range(2):
        bt = 2 * core + h
        g_copy(h).wait()
        v = jnp.where(on_chip(bt), rows[bt, 1:2, :], 0.0)
        g = (gt[2 + h] + grecv[h].astype(f32)) * rows[bt, 0:1, :] + v * ttr[h].astype(f32)
        back = transposed(g.astype(bf16))
        for p in range(4):
            gs[p, 2 * h : 2 * h + 2] = back[:, p * 128 : (p + 1) * 128].reshape(2, 4, 4, OWN, 128)

    def rs_copy(s, p, k, order):
        axis = order[2 - s]
        to = peer(axis, k)
        if s == 0:
            src = gs.at[(p,) + tuple(to[a] if a == axis else slice(None) for a in range(3))]
            dst = rb1.at[p, k - 1]
        elif s == 1:
            left = sorted(order[:2])
            src = gs2.at[(p,) + tuple(to[a] if a == axis else slice(None) for a in left)]
            dst = rb2.at[p, k - 1]
        else:
            src = gs3.at[p]
            dst = rb3.at[p, k - 1]
        return pltpu.make_async_remote_copy(
            src_ref=src, dst_ref=dst,
            send_sem=rs_send.at[s, p, k - 1], recv_sem=rs_recv.at[s, p, k - 1],
            device_id=to, device_id_type=MESH,
        )

    def rs_start(s, p):
        def act(order):
            for k in (2, 1, 3):
                rs_copy(s, p, k, order).start()

        by_order(p, act)

    def rs_step(s):
        bufs = (rb1, rb2, rb3)[s]
        for p in range(4):
            for k in (2, 1, 3):
                rs_copy(s, p, k, ORDERS[p]).wait_recv()

            def act(order):
                axis = order[2 - s]
                if s == 0:
                    total = gs[(p,) + tuple(me[a] if a == axis else slice(None) for a in range(3))]
                elif s == 1:
                    total = gs2[(p,) + tuple(me[a] if a == axis else slice(None) for a in sorted(order[:2]))]
                else:
                    total = gs3[p]
                total = total.astype(f32)
                for k in (2, 1, 3):
                    total = total + bufs[p, k - 1].astype(f32)
                if s == 0:
                    gs2[p] = total.astype(bf16)
                elif s == 1:
                    gs3[p] = total.astype(bf16)
                else:
                    where = tuple(slice(None) if a == axis else me[a] for a in range(3))
                    gemb[(p, core) + where] = total.astype(bf16)
                for k in (2, 1, 3):
                    if s < 2:
                        rs_copy(s + 1, p, k, order).start()
                    else:
                        ag_copy(gemb, 1, p, 1, k, order).start()

            by_order(p, act)

    for p in range(4):
        rs_start(0, p)

    steps = {
        2: functools.partial(rs_step, 0),
        3: functools.partial(rs_step, 1),
        5: functools.partial(rs_step, 2),
        7: functools.partial(ag_next, gemb, 1, 1),
    }

    def finish_centers(i, slot):
        r = pl.ds(pl.multiple_of(i * JC, JC), JC)
        gu = gt[slot]
        cf = cen[r, :].astype(f32)
        inv = lax.rsqrt(jnp.sum(cf * cf, axis=1, keepdims=True) + epsilon)
        along = jnp.sum(gu * cf, axis=1, keepdims=True) * (inv * inv * inv)
        gc_out[r, :] = (gu * inv - cf * along).astype(bf16)

    @pl.loop(0, CLASSES // JC)
    def _(i):
        j0 = pl.multiple_of(i * JC, JC)
        r = pl.ds(j0, JC)
        gu = jnp.zeros((JC, D), f32)
        for bt in range(4):
            lab = labels[bt : bt + 1, :] - offset - j0
            hot = lab == lax.broadcasted_iota(jnp.int32, (JC, BT), 0)
            scaled = E[bt, r, :].astype(f32) * rows[bt, 0:1, :]
            gc = jnp.where(hot, rows[bt, 1:2, :], scaled).astype(bf16)
            gu = gu + plain_dot(gc, block(emb, bt))
        gt[lax.rem(i, 2)] = gu
        before = jnp.maximum(i - 1, 0)
        finish_centers(before, lax.rem(i + 1, 2))

        for at, step in steps.items():
            @pl.when(i == at)
            def _():
                step()

    finish_centers(CLASSES // JC - 1, (CLASSES // JC - 1) % 2)
    position = core * (N // 2) + chip
    line = jnp.zeros((1, BT), f32)
    for bt in range(4):
        line = jnp.where(position // 32 == bt, losses[bt : bt + 1, :], line)
    line = jnp.broadcast_to(line, (8, BT))
    for bit in (1, 2, 4, 8, 16):
        moved = pltpu.roll(line, BT - bit * OWN, 1)
        line = jnp.where(lax.rem(position // bit, 2) == 1, moved, line)
    loss_out[...] = line[:, 0:128]

    others = cols.at[pl.ds(0, N // 2 - 1)]
    pltpu.make_async_copy(others, others, a_send).wait()
    pltpu.make_async_copy(others, others, a_recv).wait()

    start = chip * 2 * F_DEV - tile_of(chip) * 128
    r = lax.broadcasted_iota(jnp.int32, (208, 384), 0)
    want = start + jnp.where(r < 104, core * F_DEV + r, (1 - core) * F_DEV + r - 104)
    pick = (lax.broadcasted_iota(jnp.int32, (208, 384), 1) == want).astype(f32).astype(bf16)
    for h in range(2):
        cols_t[h] = last_dims(pick, cols[h * 32 : (h + 1) * 32].reshape(BT, 384)).astype(bf16)

    ag_next(gemb, 1, 2)
    tangents = []
    for h in range(2):
        grad, low = (
            jnp.concatenate([buf[p, core, 2 * h : 2 * h + 2].reshape(BT, 128) for p in range(4)], axis=1).astype(f32)
            for buf in (gemb, emb)
        )
        along = jnp.sum(grad * low, axis=1, keepdims=True)
        tangents.append((grad - low * along).astype(bf16))

    def fc_rows(start):
        return sum(plain_dot(cols_t[h, start : start + 104], tangents[h]) for h in range(2))

    fc_send[...] = fc_rows(104)
    fc_copy = pltpu.make_async_remote_copy(
        src_ref=fc_send, dst_ref=fc_recv, send_sem=d_send.at[1, 0], recv_sem=d_recv.at[1, 0],
        device_id=peer(3, 1), device_id_type=MESH,
    )
    fc_copy.start()
    fc_own = fc_rows(0)
    fc_copy.wait()
    fc_out[...] = fc_own + fc_recv[...]

    ag_drain(emb, 0)
    ag_drain(gemb, 1)
    for s in range(3):
        for p in range(4):
            for k in (2, 1, 3):
                rs_copy(s, p, k, ORDERS[p]).wait_send()


def on_device(features, fc_weight, centers, labels):
    vmem = pl.BlockSpec(memory_space=pltpu.VMEM)
    anywhere = pl.BlockSpec(memory_space=pl.ANY)
    dma = pltpu.SemaphoreType.DMA
    loss, grad_fc, grad_centers = pl.pallas_call(
        kernel,
        out_shape=(
            pltpu.VMEM((8, 128), f32),
            pltpu.VMEM((104, D), f32),
            pltpu.VMEM((CLASSES, D), bf16),
        ),
        in_specs=[anywhere] * 4,
        out_specs=(vmem, vmem, vmem),
        scratch_shapes=[
            pltpu.VMEM((OWN, F), bf16),
            pltpu.VMEM((16, 128), jnp.int32),
            pltpu.VMEM((4, BT), jnp.int32),
            pltpu.VMEM((8, BT), f32),
            pltpu.VMEM((4, CLASSES, BT), bf16),
            pltpu.VMEM((CLASSES, D), bf16),
            pltpu.VMEM((CLASSES, D), bf16),
            pltpu.VMEM((D, CLASSES), bf16),
            pltpu.VMEM((4, D, BT), bf16),
            pltpu.VMEM((2, D, BT), bf16),
            pltpu.VMEM((4, 2, 4, 4, 4, OWN, 128), bf16),
            pltpu.VMEM((4, D, BT), bf16),
            pltpu.VMEM((4, 2, 4, 4, 4, OWN, 128), bf16),
            pltpu.VMEM((4, D, BT), f32),
            pltpu.VMEM((2, D, BT), bf16),
            pltpu.VMEM((2, D, BT), bf16),
            pltpu.VMEM((4, 4, 4, 4, OWN, 128), bf16),
            pltpu.VMEM((4, 3, 4, 4, OWN, 128), bf16),
            pltpu.VMEM((4, 4, 4, OWN, 128), bf16),
            pltpu.VMEM((4, 3, 4, OWN, 128), bf16),
            pltpu.VMEM((4, 4, OWN, 128), bf16),
            pltpu.VMEM((4, 3, 4, OWN, 128), bf16),
            pltpu.VMEM((N // 2, OWN, 384), bf16),
            pltpu.VMEM((2, 208, BT), bf16),
            pltpu.VMEM((104, D), f32),
            pltpu.VMEM((104, D), f32),
            pltpu.VMEM((4, 8, BT), f32),
            pltpu.VMEM((3, 7, 8, BT), f32),
            pltpu.VMEM((4, 8, BT), f32),
            dma((N_W,)),
            dma((3,)),
            dma((2, 4, 3, 3)),
            dma((2, 4, 3, 3)),
            dma((3, 4)),
            dma((3, 4)),
            dma((3, 4, 3)),
            dma((3, 4, 3)),
            dma((3, 7)),
            dma((3, 7)),
            dma,
            dma,
        ],
        compiler_params=pltpu.CompilerParams(
            collective_id=0, has_side_effects=True, vmem_limit_bytes=58_000_000
        ),
    )(features, fc_weight, centers, labels.reshape(16, 128))
    return (loss[0, :OWN], grad_centers, grad_fc[:F_DEV])


def solution(mesh):
    torus = Mesh(mesh.devices.reshape(4, 4, 4, 2), CLS)
    placed = (P(CLS, None), P(), P(CLS, None), P())
    return jax.shard_map(
        on_device,
        mesh=torus,
        in_specs=placed,
        out_specs=(P(CLS), P(CLS, None), P(CLS, None)),
        check_vma=False,
    )
```

```python
import functools
import math

import jax
import jax.numpy as jnp
from jax import lax
from jax.experimental import pallas as pl
from jax.experimental.pallas import tpu as pltpu
from jax.sharding import Mesh
from jax.sharding import PartitionSpec as P

CLS = ("cls_0", "cls_1", "cls_2", "cls_3")
MESH = pl.DeviceIdType.MESH

logit_scale = 64.0
cos_margin = math.cos(0.5)
sin_margin = math.sin(0.5)
epsilon = 1e-06
exp2_scale = logit_scale / math.log(2.0)

N = 128
D = 512
F = 12544
F_DEV = F // N
OWN = 16
CLASSES = 4096
BT = 512
W_CHUNK = 1792
N_W = F // W_CHUNK
JA = 1024
JB = 2048
JC = 512

ORDERS = ((0, 1, 2), (1, 2, 0), (2, 0, 1), (0, 2, 1), (0, 1, 2))

f32 = jnp.float32
bf16 = jnp.bfloat16


def last_dims(a, b):
    return lax.dot_general(a, b, (((1,), (1,)), ((), ())), preferred_element_type=f32)


def plain_dot(a, b):
    return lax.dot_general(a, b, (((1,), (0,)), ((), ())), preferred_element_type=f32)


def transposed(x):
    width = x.shape[1]
    one = eye(256)
    return jnp.concatenate([last_dims(one, x[:, c : c + 256]) for c in range(0, width, 256)], axis=0).astype(bf16)


def eye(n):
    r = lax.broadcasted_iota(jnp.int32, (n, n), 0)
    c = lax.broadcasted_iota(jnp.int32, (n, n), 1)
    return (r == c).astype(f32).astype(bf16)


def kernel(
    feat_hbm, w_hbm, centers_hbm, labels_hbm,
    loss_out, fc_out, gc_out,
    feat, labels_in, labels, losses,
    E, cen, clow, ct, tt, ttr, emb, emb_t, gemb, gt, gsend, grecv, gs, rb1, gs2, rb2, gs3, rb3, cols,
    cols_t, fc_send, fc_recv, ar_send, ar_recv, rows,
    w_sem, c_sem, ag_send, ag_recv, d_send, d_recv, rs_send, rs_recv,
    s_send, s_recv, a_send, a_recv,
):
    me = tuple(lax.axis_index(name) for name in CLS)
    core = me[3]
    idx = ((me[0] * 4 + me[1]) * 4 + me[2]) * 2 + core
    offset = idx * CLASSES
    chip = idx // 2

    def peer(axis, k):
        size = 2 if axis == 3 else 4
        coords = list(me)
        coords[axis] = lax.rem(me[axis] + k, size)
        return tuple(coords)

    def w_copy(i):
        return pltpu.make_async_copy(
            w_hbm.at[pl.ds(i * W_CHUNK, W_CHUNK)],
            E.at[i // 2, pl.ds((i % 2) * 2048, W_CHUNK)],
            w_sem.at[i],
        )

    feat_fetch = pltpu.make_async_copy(feat_hbm, feat, c_sem.at[1])
    labels_fetch = pltpu.make_async_copy(labels_hbm, labels_in, c_sem.at[2])
    c_copy = pltpu.make_async_copy(centers_hbm, cen, c_sem.at[0])
    feat_fetch.start()
    labels_fetch.start()
    for i in range(N_W):
        w_copy(i).start()
    c_copy.start()

    barrier = pltpu.get_barrier_semaphore()
    for axis in range(3):
        for k in (2, 1, 3):
            pl.semaphore_signal(barrier, inc=1, device_id=peer(axis, k), device_id_type=MESH)
    pl.semaphore_signal(barrier, inc=1, device_id=peer(3, 1), device_id_type=MESH)

    labels_fetch.wait()
    lane = lax.broadcasted_iota(jnp.int32, (16, 128), 1)
    for c in range(2):
        low = labels_in[...]
        for m in range(4):
            moved = pltpu.roll(labels_in[...], (-16 * m - 16 * c) % 128, 1)
            low = jnp.where(lane // 16 == m, moved, low)
        high = pltpu.roll(low, 64, 1)
        for g in range(8):
            line = jnp.where(lane[0:1] < 64, low[2 * g : 2 * g + 1], high[2 * g + 1 : 2 * g + 2])
            labels[2 * c + g // 4 : 2 * c + g // 4 + 1, (g % 4) * 128 : (g % 4 + 1) * 128] = line

    feat_fetch.wait()
    acc = jnp.zeros((OWN, D), f32)
    for i in range(N_W):
        w_copy(i).wait()
        at = (i % 2) * 2048
        acc = acc + plain_dot(feat[:, i * W_CHUNK : (i + 1) * W_CHUNK], E[i // 2, at : at + W_CHUNK])
    own = acc.astype(bf16).astype(f32)
    own_inv = lax.rsqrt(jnp.sum(own * own, axis=1, keepdims=True) + epsilon)
    own_low = (own * own_inv).astype(bf16)

    def put_own(buf, value):
        for p in range(4):
            buf[p, core, me[0], me[1], me[2]] = value[:, p * 128 : (p + 1) * 128]

    def view(buf, p, gathered, at=None):
        at = me if at is None else at
        where = tuple(slice(None) if a in gathered else at[a] for a in range(3))
        return buf.at[(p, core) + where]

    def wait_bytes(ref, sem):
        pltpu.make_async_copy(ref, ref, sem).wait()

    def by_order(p, act):
        if p < 3:
            act(ORDERS[p])
            return
        for c in range(2):
            @pl.when(core == c)
            def _():
                act(ORDERS[3 + c])

    def ag_copy(buf, inst, p, s, k, order):
        v = view(buf, p, order[:s])
        return pltpu.make_async_remote_copy(
            src_ref=v, dst_ref=v,
            send_sem=ag_send.at[inst, s], recv_sem=ag_recv.at[inst, p, s],
            device_id=peer(order[s], k), device_id_type=MESH,
        )

    def ag_start(buf, inst, p, s):
        def act(order):
            for k in (2, 1, 3):
                ag_copy(buf, inst, p, s, k, order).start()

        by_order(p, act)

    def ag_next(buf, inst, s):
        for p in range(4):
            first = buf.at[p, 0]
            wait_bytes((first.at[0, 0, 0:3], first.at[0, 0:3], first.at[0:3])[s], ag_recv.at[inst, p, s])
            if s < 2:
                ag_start(buf, inst, p, s + 1)
            elif inst == 0:
                pair_copy(buf, inst, p).start()

    def ag_drain(buf, inst):
        sizes = (buf.at[:, 0, 0, 0, 0:3], buf.at[:, 0, 0, 0:3], buf.at[:, 0, 0:3])
        for s in range(inst, 3):
            wait_bytes(sizes[s], ag_send.at[inst, s])

    def pair_copy(buf, inst, p):
        v = buf.at[p, core]
        return pltpu.make_async_remote_copy(
            src_ref=v, dst_ref=v,
            send_sem=d_send.at[inst, p], recv_sem=d_recv.at[inst, p],
            device_id=peer(3, 1), device_id_type=MESH,
        )

    def pair_wait(buf, inst):
        for p in range(4):
            pair_copy(buf, inst, p).wait()

    def block(buf, bt):
        c, y0 = bt // 2, (bt % 2) * 2
        return jnp.concatenate([buf[p, c, pl.ds(y0, 2)].reshape(BT, 128) for p in range(4)], axis=1)

    put_own(emb, own_low)
    pl.semaphore_wait(barrier, 10)
    for p in range(4):
        ag_start(emb, 0, p, 0)

    feat[...] = (feat[...].astype(f32) * own_inv).astype(bf16)

    c_copy.wait()

    @pl.loop(0, CLASSES // JC)
    def _(i):
        r = pl.ds(pl.multiple_of(i * JC, JC), JC)
        cf = cen[r, :].astype(f32)
        inv = lax.rsqrt(jnp.sum(cf * cf, axis=1, keepdims=True) + epsilon)
        low = (cf * inv).astype(bf16)
        clow[r, :] = low
        ct[:, r] = transposed(low)

        @pl.when(i == 5)
        def _():
            ag_next(emb, 0, 0)

    @pl.loop(0, 4)
    def _(bt):
        lab = labels[pl.ds(bt, 1), :] - offset
        total = jnp.zeros((D, BT), f32)
        for j0 in range(0, CLASSES, JB):
            hot = (lab - j0) == lax.broadcasted_iota(jnp.int32, (JB, BT), 0)
            hot = jnp.where(hot, 1.0, 0.0).astype(bf16)
            total = total + plain_dot(ct[:, j0 : j0 + JB], hot)
        tt[bt] = total.astype(bf16)

        @pl.when(bt == 0)
        def _():
            ag_next(emb, 0, 1)

    ag_next(emb, 0, 2)

    def tt_copy():
        return pltpu.make_async_remote_copy(
            src_ref=tt.at[pl.ds(2 * (1 - core), 2)], dst_ref=ttr,
            send_sem=d_send.at[1, 1], recv_sem=d_recv.at[1, 1], device_id=peer(3, 1), device_id_type=MESH,
        )

    tt_copy().start()
    def tile_of(c):
        return jnp.minimum((c * 2 * F_DEV) // 128, F // 128 - 3)

    def feature_copy(k):
        to = lax.bitwise_and(chip + k, N // 2 - 1)
        coords = (
            lax.shift_right_logical(to, 4), lax.bitwise_and(lax.shift_right_logical(to, 2), 3), lax.bitwise_and(to, 3), core
        )
        return pltpu.make_async_remote_copy(
            src_ref=feat.at[:, pl.ds(pl.multiple_of(tile_of(to) * 128, 128), 384)],
            dst_ref=cols.at[chip],
            send_sem=a_send, recv_sem=a_recv, device_id=coords, device_id_type=MESH,
        )

    cols[chip] = feat[:, pl.ds(pl.multiple_of(tile_of(chip) * 128, 128), 384)]

    rows[...] = jnp.zeros_like(rows)
    n_a = CLASSES // JA

    def side(n):
        return lax.rem(n + 2 * core, 4)

    def turn(n):
        emb_t[side(n)] = transposed(block(emb, side(n)))

    def cosine_tile(n, a):
        slot = 2 * (a % 2)
        gt[slot : slot + 2] = plain_dot(clow[a * JA : (a + 1) * JA, :], emb_t[side(n)]).reshape(2, BT, BT)

    def exp_tile(n, a):
        slot = 2 * (a % 2)
        cosines = gt[slot : slot + 2].reshape(JA, BT)
        lab = labels[pl.ds(side(n), 1), :] - offset - a * JA
        hot = lab == lax.broadcasted_iota(jnp.int32, (JA, BT), 0)
        e = jnp.where(hot, 0.0, jnp.exp2(cosines * exp2_scale))
        rows[side(n)] += jnp.sum(e.reshape(JA // 8, 8, BT), axis=0)
        E[side(n), a * JA : (a + 1) * JA, :] = e.astype(bf16)

    turn(0)
    turn(1)
    cosine_tile(0, 0)

    @pl.loop(0, 3)
    def _(n):
        @pl.when(n == 1)
        def _():
            pair_wait(emb, 0)
            turn(2)
            turn(3)

        for u in range(21):
            feature_copy(n * 21 + u + 1).start()
        for a in range(n_a):
            if a + 1 < n_a:
                cosine_tile(n, a + 1)
            else:
                cosine_tile(n + 1, 0)
            exp_tile(n, a)

    for a in range(n_a):
        if a + 1 < n_a:
            cosine_tile(3, a + 1)
        exp_tile(3, a)

    def margin(tc):
        ts = jnp.sqrt(1.0 - tc * tc)
        margined = logit_scale * (tc * cos_margin - ts * sin_margin)
        return margined, cos_margin + sin_margin * tc / ts

    def on_chip(bt):
        lab = labels[pl.ds(bt, 1), :] - chip * (2 * CLASSES)
        return jnp.logical_and(lab >= 0, lab < 2 * CLASSES)

    ar_send[0, 4:8, :] = jnp.zeros((4, BT), f32)
    for bt in range(4):
        ar_send[0, bt : bt + 1, :] = jnp.sum(rows[bt], axis=0, keepdims=True)
    tt_copy().wait()
    for h in range(2):
        bt = 2 * core + h
        rows_t = tt[bt].astype(f32) + ttr[h].astype(f32)
        ttr[h] = rows_t.astype(bf16)
        tc = jnp.sum(emb_t[bt].astype(f32) * rows_t, axis=0, keepdims=True)
        margined, _ = margin(tc)
        ar_send[0, pl.ds(bt, 1), :] += jnp.where(on_chip(bt), jnp.exp(margined), 0.0)
        ar_send[0, pl.ds(4 + bt, 1), :] = tc

    AR_PEERS = (
        tuple((z, c) for z in (2, 1, 3, 0) for c in range(2) if z + c > 0),
        tuple((1, k) for k in (2, 1, 3)),
        tuple((0, k) for k in (2, 1, 3)),
    )

    def ar_copy(s, n):
        if s == 0:
            dz, dc = AR_PEERS[0][n]
            to = (me[0], me[1], lax.rem(me[2] + dz, 4), lax.rem(core + dc, 2))
        else:
            to = peer(*AR_PEERS[s][n])
        return pltpu.make_async_remote_copy(
            src_ref=ar_send.at[s], dst_ref=ar_recv.at[s, n],
            send_sem=s_send.at[s], recv_sem=s_recv.at[s],
            device_id=to, device_id_type=MESH,
        )

    def ar_start(s):
        for n in range(len(AR_PEERS[s])):
            ar_copy(s, n).start()

    def ar_finish(s):
        total = ar_send[s]
        wait_bytes(ar_recv.at[s, 0 : len(AR_PEERS[s])], s_recv.at[s])
        for n in range(len(AR_PEERS[s])):
            total = total + ar_recv[s, n]
        ar_send[s + 1] = total
        if s < 2:
            ar_start(s + 1)

    ar_start(0)

    def g_copy(h):
        return pltpu.make_async_remote_copy(
            src_ref=gsend.at[h], dst_ref=grecv.at[h],
            send_sem=d_send.at[2, h], recv_sem=d_recv.at[2, h], device_id=peer(3, 1), device_id_type=MESH,
        )

    half = CLASSES // 2

    @pl.loop(0, 4)
    def _(i):
        bt = lax.rem(i + 2 * core + 2, 4)
        gt[i] = plain_dot(ct[:, 0:half], E[bt, 0:half, :])

        @pl.when(i == 1)
        def _():
            ar_finish(0)

        gt[i] += plain_dot(ct[:, half:], E[bt, half:, :])

        @pl.when(i == 2)
        def _():
            ar_finish(1)

        @pl.when(i < 2)
        def _():
            gsend[i] = gt[i].astype(bf16)
            g_copy(i).start()

    ar_finish(2)
    for s in range(3):
        wait_bytes(ar_recv.at[s, 0 : len(AR_PEERS[s])], s_send.at[s])

    for bt in range(4):
        total = ar_send[3, bt : bt + 1, :]
        margined, slope = margin(ar_send[3, 4 + bt : 5 + bt, :])
        losses[bt : bt + 1, :] = jnp.log(total) - margined
        scale = logit_scale / total
        rows[bt, 0:1, :] = scale
        rows[bt, 1:2, :] = (jnp.exp(margined) - total) * slope * scale

    for h in range(2):
        bt = 2 * core + h
        g_copy(h).wait()
        v = jnp.where(on_chip(bt), rows[bt, 1:2, :], 0.0)
        g = (gt[2 + h] + grecv[h].astype(f32)) * rows[bt, 0:1, :] + v * ttr[h].astype(f32)
        back = transposed(g.astype(bf16))
        for p in range(4):
            gs[p, 2 * h : 2 * h + 2] = back[:, p * 128 : (p + 1) * 128].reshape(2, 4, 4, OWN, 128)

    def rs_copy(s, p, k, order):
        axis = order[2 - s]
        to = peer(axis, k)
        if s == 0:
            src = gs.at[(p,) + tuple(to[a] if a == axis else slice(None) for a in range(3))]
            dst = rb1.at[p, k - 1]
        elif s == 1:
            left = sorted(order[:2])
            src = gs2.at[(p,) + tuple(to[a] if a == axis else slice(None) for a in left)]
            dst = rb2.at[p, k - 1]
        else:
            src = gs3.at[p]
            dst = rb3.at[p, k - 1]
        return pltpu.make_async_remote_copy(
            src_ref=src, dst_ref=dst,
            send_sem=rs_send.at[s], recv_sem=rs_recv.at[s, p],
            device_id=to, device_id_type=MESH,
        )

    def rs_start(s, p):
        def act(order):
            for k in (2, 1, 3):
                rs_copy(s, p, k, order).start()

        by_order(p, act)

    def rs_step(s):
        bufs = (rb1, rb2, rb3)[s]
        for p in range(4):
            wait_bytes(bufs.at[p], rs_recv.at[s, p])

            def act(order):
                axis = order[2 - s]
                if s == 0:
                    total = gs[(p,) + tuple(me[a] if a == axis else slice(None) for a in range(3))]
                elif s == 1:
                    total = gs2[(p,) + tuple(me[a] if a == axis else slice(None) for a in sorted(order[:2]))]
                else:
                    total = gs3[p]
                total = total.astype(f32)
                for k in (2, 1, 3):
                    total = total + bufs[p, k - 1].astype(f32)
                if s == 0:
                    gs2[p] = total.astype(bf16)
                elif s == 1:
                    gs3[p] = total.astype(bf16)
                else:
                    where = tuple(slice(None) if a == axis else me[a] for a in range(3))
                    gemb[(p, core) + where] = total.astype(bf16)
                for k in (2, 1, 3):
                    if s < 2:
                        rs_copy(s + 1, p, k, order).start()
                    else:
                        ag_copy(gemb, 1, p, 1, k, order).start()

            by_order(p, act)

    for p in range(4):
        rs_start(0, p)

    steps = {
        2: functools.partial(rs_step, 0),
        3: functools.partial(rs_step, 1),
        5: functools.partial(rs_step, 2),
        7: functools.partial(ag_next, gemb, 1, 1),
    }

    def finish_centers(i, slot):
        r = pl.ds(pl.multiple_of(i * JC, JC), JC)
        gu = gt[slot]
        cf = cen[r, :].astype(f32)
        inv = lax.rsqrt(jnp.sum(cf * cf, axis=1, keepdims=True) + epsilon)
        along = jnp.sum(gu * cf, axis=1, keepdims=True) * (inv * inv * inv)
        gc_out[r, :] = (gu * inv - cf * along).astype(bf16)

    @pl.loop(0, CLASSES // JC)
    def _(i):
        j0 = pl.multiple_of(i * JC, JC)
        r = pl.ds(j0, JC)
        gu = jnp.zeros((JC, D), f32)
        for bt in range(4):
            lab = labels[bt : bt + 1, :] - offset - j0
            hot = lab == lax.broadcasted_iota(jnp.int32, (JC, BT), 0)
            scaled = E[bt, r, :].astype(f32) * rows[bt, 0:1, :]
            gc = jnp.where(hot, rows[bt, 1:2, :], scaled).astype(bf16)
            gu = gu + plain_dot(gc, block(emb, bt))
        gt[lax.rem(i, 2)] = gu
        before = jnp.maximum(i - 1, 0)
        finish_centers(before, lax.rem(i + 1, 2))

        for at, step in steps.items():
            @pl.when(i == at)
            def _():
                step()

    finish_centers(CLASSES // JC - 1, (CLASSES // JC - 1) % 2)
    position = core * (N // 2) + chip
    line = jnp.zeros((1, BT), f32)
    for bt in range(4):
        line = jnp.where(position // 32 == bt, losses[bt : bt + 1, :], line)
    line = jnp.broadcast_to(line, (8, BT))
    for bit in (1, 2, 4, 8, 16):
        moved = pltpu.roll(line, BT - bit * OWN, 1)
        line = jnp.where(lax.rem(position // bit, 2) == 1, moved, line)
    loss_out[...] = line[:, 0:128]

    others = cols.at[pl.ds(0, N // 2 - 1)]
    pltpu.make_async_copy(others, others, a_send).wait()
    pltpu.make_async_copy(others, others, a_recv).wait()

    start = chip * 2 * F_DEV - tile_of(chip) * 128
    r = lax.broadcasted_iota(jnp.int32, (208, 384), 0)
    want = start + jnp.where(r < 104, core * F_DEV + r, (1 - core) * F_DEV + r - 104)
    pick = (lax.broadcasted_iota(jnp.int32, (208, 384), 1) == want).astype(f32).astype(bf16)
    for h in range(2):
        cols_t[h] = last_dims(pick, cols[h * 32 : (h + 1) * 32].reshape(BT, 384)).astype(bf16)

    ag_next(gemb, 1, 2)
    tangents = []
    for h in range(2):
        grad, low = (
            jnp.concatenate([buf[p, core, 2 * h : 2 * h + 2].reshape(BT, 128) for p in range(4)], axis=1).astype(f32)
            for buf in (gemb, emb)
        )
        along = jnp.sum(grad * low, axis=1, keepdims=True)
        tangents.append((grad - low * along).astype(bf16))

    def fc_rows(start):
        return sum(plain_dot(cols_t[h, start : start + 104], tangents[h]) for h in range(2))

    fc_send[...] = fc_rows(104)
    fc_copy = pltpu.make_async_remote_copy(
        src_ref=fc_send, dst_ref=fc_recv, send_sem=d_send.at[1, 0], recv_sem=d_recv.at[1, 0],
        device_id=peer(3, 1), device_id_type=MESH,
    )
    fc_copy.start()
    fc_own = fc_rows(0)
    fc_copy.wait()
    fc_out[...] = fc_own + fc_recv[...]

    ag_drain(emb, 0)
    ag_drain(gemb, 1)
    for s in range(3):
        wait_bytes((rb1, rb2, rb3)[s], rs_send.at[s])


def on_device(features, fc_weight, centers, labels):
    vmem = pl.BlockSpec(memory_space=pltpu.VMEM)
    anywhere = pl.BlockSpec(memory_space=pl.ANY)
    dma = pltpu.SemaphoreType.DMA
    loss, grad_fc, grad_centers = pl.pallas_call(
        kernel,
        out_shape=(
            pltpu.VMEM((8, 128), f32),
            pltpu.VMEM((104, D), f32),
            pltpu.VMEM((CLASSES, D), bf16),
        ),
        in_specs=[anywhere] * 4,
        out_specs=(vmem, vmem, vmem),
        scratch_shapes=[
            pltpu.VMEM((OWN, F), bf16),
            pltpu.VMEM((16, 128), jnp.int32),
            pltpu.VMEM((16, BT), jnp.int32),
            pltpu.VMEM((8, BT), f32),
            pltpu.VMEM((4, CLASSES, BT), bf16),
            pltpu.VMEM((CLASSES, D), bf16),
            pltpu.VMEM((CLASSES, D), bf16),
            pltpu.VMEM((D, CLASSES), bf16),
            pltpu.VMEM((4, D, BT), bf16),
            pltpu.VMEM((2, D, BT), bf16),
            pltpu.VMEM((4, 2, 4, 4, 4, OWN, 128), bf16),
            pltpu.VMEM((4, D, BT), bf16),
            pltpu.VMEM((4, 2, 4, 4, 4, OWN, 128), bf16),
            pltpu.VMEM((4, D, BT), f32),
            pltpu.VMEM((2, D, BT), bf16),
            pltpu.VMEM((2, D, BT), bf16),
            pltpu.VMEM((4, 4, 4, 4, OWN, 128), bf16),
            pltpu.VMEM((4, 3, 4, 4, OWN, 128), bf16),
            pltpu.VMEM((4, 4, 4, OWN, 128), bf16),
            pltpu.VMEM((4, 3, 4, OWN, 128), bf16),
            pltpu.VMEM((4, 4, OWN, 128), bf16),
            pltpu.VMEM((4, 3, 4, OWN, 128), bf16),
            pltpu.VMEM((N // 2, OWN, 384), bf16),
            pltpu.VMEM((2, 208, BT), bf16),
            pltpu.VMEM((104, D), f32),
            pltpu.VMEM((104, D), f32),
            pltpu.VMEM((4, 8, BT), f32),
            pltpu.VMEM((3, 7, 8, BT), f32),
            pltpu.VMEM((4, 8, BT), f32),
            dma((N_W,)),
            dma((3,)),
            dma((2, 3)),
            dma((2, 4, 3)),
            dma((3, 4)),
            dma((3, 4)),
            dma((3,)),
            dma((3, 4)),
            dma((3,)),
            dma((3,)),
            dma,
            dma,
        ],
        compiler_params=pltpu.CompilerParams(
            collective_id=0, has_side_effects=True, vmem_limit_bytes=58_000_000
        ),
    )(features, fc_weight, centers, labels.reshape(16, 128))
    return (loss[0, :OWN], grad_centers, grad_fc[:F_DEV])


def solution(mesh):
    torus = Mesh(mesh.devices.reshape(4, 4, 4, 2), CLS)
    placed = (P(CLS, None), P(), P(CLS, None), P())
    return jax.shard_map(
        on_device,
        mesh=torus,
        in_specs=placed,
        out_specs=(P(CLS), P(CLS, None), P(CLS, None)),
        check_vma=False,
    )
```

```python
import functools
import math

import jax
import jax.numpy as jnp
from jax import lax
from jax.experimental import pallas as pl
from jax.experimental.pallas import tpu as pltpu
from jax.sharding import Mesh
from jax.sharding import PartitionSpec as P

CLS = ("cls_0", "cls_1", "cls_2", "cls_3")
MESH = pl.DeviceIdType.MESH

logit_scale = 64.0
cos_margin = math.cos(0.5)
sin_margin = math.sin(0.5)
epsilon = 1e-06
exp2_scale = logit_scale / math.log(2.0)

N = 128
D = 512
F = 12544
F_DEV = F // N
OWN = 16
CLASSES = 4096
BT = 512
W_CHUNK = 1792
N_W = F // W_CHUNK
JA = 1024
JB = 2048
JC = 512

ORDERS = ((0, 1, 2), (1, 2, 0), (2, 0, 1), (0, 2, 1), (0, 1, 2))

f32 = jnp.float32
bf16 = jnp.bfloat16


def last_dims(a, b):
    return lax.dot_general(a, b, (((1,), (1,)), ((), ())), preferred_element_type=f32)


def plain_dot(a, b):
    return lax.dot_general(a, b, (((1,), (0,)), ((), ())), preferred_element_type=f32)


def transposed(x):
    width = x.shape[1]
    one = eye(256)
    return jnp.concatenate([last_dims(one, x[:, c : c + 256]) for c in range(0, width, 256)], axis=0).astype(bf16)


def eye(n):
    r = lax.broadcasted_iota(jnp.int32, (n, n), 0)
    c = lax.broadcasted_iota(jnp.int32, (n, n), 1)
    return (r == c).astype(f32).astype(bf16)


def kernel(
    feat_hbm, w_hbm, centers_hbm, labels_hbm,
    loss_out, fc_out, gc_out,
    feat, labels_in, labels, losses,
    E, cen, clow, ct, tt, ttr, emb, emb_t, gemb, gt, gsend, grecv, gs, rb1, gs2, rb2, gs3, rb3, cols,
    cols_t, fc_send, fc_recv, ar_send, ar_recv, rows,
    w_sem, c_sem, ag_send, ag_recv, d_send, d_recv, rs_send, rs_recv,
    s_send, s_recv, a_send, a_recv,
):
    me = tuple(lax.axis_index(name) for name in CLS)
    core = me[3]
    idx = ((me[0] * 4 + me[1]) * 4 + me[2]) * 2 + core
    offset = idx * CLASSES
    chip = idx // 2

    def peer(axis, k):
        size = 2 if axis == 3 else 4
        coords = list(me)
        coords[axis] = lax.rem(me[axis] + k, size)
        return tuple(coords)

    def w_copy(i):
        return pltpu.make_async_copy(
            w_hbm.at[pl.ds(i * W_CHUNK, W_CHUNK)],
            E.at[i // 2, pl.ds((i % 2) * 2048, W_CHUNK)],
            w_sem.at[i],
        )

    feat_fetch = pltpu.make_async_copy(feat_hbm, feat, c_sem.at[1])
    labels_fetch = pltpu.make_async_copy(labels_hbm, labels_in, c_sem.at[2])
    c_copy = pltpu.make_async_copy(centers_hbm, cen, c_sem.at[0])
    feat_fetch.start()
    labels_fetch.start()
    for i in range(N_W):
        w_copy(i).start()
    c_copy.start()

    barrier = pltpu.get_barrier_semaphore()
    for axis in range(3):
        for k in (2, 1, 3):
            pl.semaphore_signal(barrier, inc=1, device_id=peer(axis, k), device_id_type=MESH)
    pl.semaphore_signal(barrier, inc=1, device_id=peer(3, 1), device_id_type=MESH)

    labels_fetch.wait()
    lane = lax.broadcasted_iota(jnp.int32, (16, 128), 1)
    for c in range(2):
        low = labels_in[...]
        for m in range(4):
            moved = pltpu.roll(labels_in[...], (-16 * m - 16 * c) % 128, 1)
            low = jnp.where(lane // 16 == m, moved, low)
        high = pltpu.roll(low, 64, 1)
        for g in range(8):
            line = jnp.where(lane[0:1] < 64, low[2 * g : 2 * g + 1], high[2 * g + 1 : 2 * g + 2])
            labels[2 * c + g // 4 : 2 * c + g // 4 + 1, (g % 4) * 128 : (g % 4 + 1) * 128] = line

    feat_fetch.wait()
    acc = jnp.zeros((OWN, D), f32)
    for i in range(N_W):
        w_copy(i).wait()
        at = (i % 2) * 2048
        acc = acc + plain_dot(feat[:, i * W_CHUNK : (i + 1) * W_CHUNK], E[i // 2, at : at + W_CHUNK])
    own = acc.astype(bf16).astype(f32)
    own_inv = lax.rsqrt(jnp.sum(own * own, axis=1, keepdims=True) + epsilon)
    own_low = (own * own_inv).astype(bf16)

    def put_own(buf, value):
        for p in range(4):
            buf[p, core, me[0], me[1], me[2]] = value[:, p * 128 : (p + 1) * 128]

    def view(buf, p, gathered, at=None):
        at = me if at is None else at
        where = tuple(slice(None) if a in gathered else at[a] for a in range(3))
        return buf.at[(p, core) + where]

    def wait_bytes(ref, sem):
        pltpu.make_async_copy(ref, ref, sem).wait()

    def by_order(p, act):
        if p < 3:
            act(ORDERS[p])
            return
        for c in range(2):
            @pl.when(core == c)
            def _():
                act(ORDERS[3 + c])

    def ag_copy(buf, inst, p, s, k, order):
        v = view(buf, p, order[:s])
        return pltpu.make_async_remote_copy(
            src_ref=v, dst_ref=v,
            send_sem=ag_send.at[inst, s], recv_sem=ag_recv.at[inst, p, s],
            device_id=peer(order[s], k), device_id_type=MESH,
        )

    def ag_start(buf, inst, p, s):
        def act(order):
            for k in (2, 1, 3):
                ag_copy(buf, inst, p, s, k, order).start()

        by_order(p, act)

    def ag_next(buf, inst, s):
        for p in range(4):
            first = buf.at[p, 0]
            wait_bytes((first.at[0, 0, 0:3], first.at[0, 0:3], first.at[0:3])[s], ag_recv.at[inst, p, s])
            if s < 2:
                ag_start(buf, inst, p, s + 1)
            elif inst == 0:
                pair_copy(buf, inst, p).start()

    def ag_drain(buf, inst):
        sizes = (buf.at[:, 0, 0, 0, 0:3], buf.at[:, 0, 0, 0:3], buf.at[:, 0, 0:3])
        for s in range(inst, 3):
            wait_bytes(sizes[s], ag_send.at[inst, s])

    def pair_copy(buf, inst, p):
        v = buf.at[p, core]
        return pltpu.make_async_remote_copy(
            src_ref=v, dst_ref=v,
            send_sem=d_send.at[0], recv_sem=d_recv.at[0],
            device_id=peer(3, 1), device_id_type=MESH,
        )

    def pair_wait(buf, inst):
        wait_bytes(buf.at[:, 0], d_send.at[0])
        wait_bytes(buf.at[:, 0], d_recv.at[0])

    def block(buf, bt):
        c, y0 = bt // 2, (bt % 2) * 2
        return jnp.concatenate([buf[p, c, pl.ds(y0, 2)].reshape(BT, 128) for p in range(4)], axis=1)

    put_own(emb, own_low)
    pl.semaphore_wait(barrier, 10)
    for p in range(4):
        ag_start(emb, 0, p, 0)

    feat[...] = (feat[...].astype(f32) * own_inv).astype(bf16)

    c_copy.wait()

    @pl.loop(0, CLASSES // JC)
    def _(i):
        r = pl.ds(pl.multiple_of(i * JC, JC), JC)
        cf = cen[r, :].astype(f32)
        inv = lax.rsqrt(jnp.sum(cf * cf, axis=1, keepdims=True) + epsilon)
        low = (cf * inv).astype(bf16)
        clow[r, :] = low
        ct[:, r] = transposed(low)

        @pl.when(i == 5)
        def _():
            ag_next(emb, 0, 0)

    @pl.loop(0, 4)
    def _(bt):
        lab = labels[pl.ds(bt, 1), :] - offset
        total = jnp.zeros((D, BT), f32)
        for j0 in range(0, CLASSES, JB):
            hot = (lab - j0) == lax.broadcasted_iota(jnp.int32, (JB, BT), 0)
            hot = jnp.where(hot, 1.0, 0.0).astype(bf16)
            total = total + plain_dot(ct[:, j0 : j0 + JB], hot)
        tt[bt] = total.astype(bf16)

        @pl.when(bt == 0)
        def _():
            ag_next(emb, 0, 1)

    ag_next(emb, 0, 2)

    def tt_copy():
        return pltpu.make_async_remote_copy(
            src_ref=tt.at[pl.ds(2 * (1 - core), 2)], dst_ref=ttr,
            send_sem=d_send.at[1], recv_sem=d_recv.at[1], device_id=peer(3, 1), device_id_type=MESH,
        )

    tt_copy().start()
    def tile_of(c):
        return jnp.minimum(lax.div(c * (2 * F_DEV), 128), F // 128 - 3)

    def feature_copy(k):
        to = lax.bitwise_and(chip + k, N // 2 - 1)
        coords = (
            lax.shift_right_logical(to, 4), lax.bitwise_and(lax.shift_right_logical(to, 2), 3), lax.bitwise_and(to, 3), core
        )
        return pltpu.make_async_remote_copy(
            src_ref=feat.at[:, pl.ds(pl.multiple_of(tile_of(to) * 128, 128), 384)],
            dst_ref=cols.at[chip],
            send_sem=a_send, recv_sem=a_recv, device_id=coords, device_id_type=MESH,
        )

    cols[chip] = feat[:, pl.ds(pl.multiple_of(tile_of(chip) * 128, 128), 384)]

    rows[...] = jnp.zeros_like(rows)
    n_a = CLASSES // JA

    def side(n):
        return lax.rem(n + 2 * core, 4)

    def turn(n):
        emb_t[side(n)] = transposed(block(emb, side(n)))

    def cosine_tile(n, a):
        slot = 2 * (a % 2)
        gt[slot : slot + 2] = plain_dot(clow[a * JA : (a + 1) * JA, :], emb_t[side(n)]).reshape(2, BT, BT)

    def exp_tile(n, a):
        slot = 2 * (a % 2)
        cosines = gt[slot : slot + 2].reshape(JA, BT)
        lab = labels[pl.ds(side(n), 1), :] - offset - a * JA
        hot = lab == lax.broadcasted_iota(jnp.int32, (JA, BT), 0)
        e = jnp.where(hot, 0.0, jnp.exp2(cosines * exp2_scale))
        rows[side(n)] += jnp.sum(e.reshape(JA // 8, 8, BT), axis=0)
        E[side(n), a * JA : (a + 1) * JA, :] = e.astype(bf16)

    turn(0)
    turn(1)
    cosine_tile(0, 0)

    @pl.loop(0, 3)
    def _(n):
        @pl.when(n == 1)
        def _():
            pair_wait(emb, 0)
            turn(2)
            turn(3)

        for u in range(21):
            feature_copy(n * 21 + u + 1).start()
        for a in range(n_a):
            if a + 1 < n_a:
                cosine_tile(n, a + 1)
            else:
                cosine_tile(n + 1, 0)
            exp_tile(n, a)

    for a in range(n_a):
        if a + 1 < n_a:
            cosine_tile(3, a + 1)
        exp_tile(3, a)

    def margin(tc):
        ts = jnp.sqrt(1.0 - tc * tc)
        margined = logit_scale * (tc * cos_margin - ts * sin_margin)
        return margined, cos_margin + sin_margin * tc / ts

    def on_chip(bt):
        lab = labels[pl.ds(bt, 1), :] - chip * (2 * CLASSES)
        return jnp.logical_and(lab >= 0, lab < 2 * CLASSES)

    ar_send[0, 4:8, :] = jnp.zeros((4, BT), f32)
    for bt in range(4):
        ar_send[0, bt : bt + 1, :] = jnp.sum(rows[bt], axis=0, keepdims=True)
    tt_copy().wait()
    for h in range(2):
        bt = 2 * core + h
        rows_t = tt[bt].astype(f32) + ttr[h].astype(f32)
        ttr[h] = rows_t.astype(bf16)
        tc = jnp.sum(emb_t[bt].astype(f32) * rows_t, axis=0, keepdims=True)
        margined, _ = margin(tc)
        ar_send[0, pl.ds(bt, 1), :] += jnp.where(on_chip(bt), jnp.exp(margined), 0.0)
        ar_send[0, pl.ds(4 + bt, 1), :] = tc

    AR_PEERS = (
        tuple((z, c) for z in (2, 1, 3, 0) for c in range(2) if z + c > 0),
        tuple((1, k) for k in (2, 1, 3)),
        tuple((0, k) for k in (2, 1, 3)),
    )

    def ar_copy(s, n):
        if s == 0:
            dz, dc = AR_PEERS[0][n]
            to = (me[0], me[1], lax.rem(me[2] + dz, 4), lax.rem(core + dc, 2))
        else:
            to = peer(*AR_PEERS[s][n])
        return pltpu.make_async_remote_copy(
            src_ref=ar_send.at[s], dst_ref=ar_recv.at[s, n],
            send_sem=s_send.at[s], recv_sem=s_recv.at[s],
            device_id=to, device_id_type=MESH,
        )

    def ar_start(s):
        for n in range(len(AR_PEERS[s])):
            ar_copy(s, n).start()

    def ar_finish(s):
        total = ar_send[s]
        wait_bytes(ar_recv.at[s, 0 : len(AR_PEERS[s])], s_recv.at[s])
        for n in range(len(AR_PEERS[s])):
            total = total + ar_recv[s, n]
        ar_send[s + 1] = total
        if s < 2:
            ar_start(s + 1)

    ar_start(0)

    def g_copy(h):
        return pltpu.make_async_remote_copy(
            src_ref=gsend.at[h], dst_ref=grecv.at[h],
            send_sem=d_send.at[2 + h], recv_sem=d_recv.at[2 + h], device_id=peer(3, 1), device_id_type=MESH,
        )

    half = CLASSES // 2

    @pl.loop(0, 4)
    def _(i):
        bt = lax.rem(i + 2 * core + 2, 4)
        gt[i] = plain_dot(ct[:, 0:half], E[bt, 0:half, :])

        @pl.when(i == 1)
        def _():
            ar_finish(0)

        gt[i] += plain_dot(ct[:, half:], E[bt, half:, :])

        @pl.when(i == 2)
        def _():
            ar_finish(1)

        @pl.when(i < 2)
        def _():
            gsend[i] = gt[i].astype(bf16)
            g_copy(i).start()

    ar_finish(2)
    for s in range(3):
        wait_bytes(ar_recv.at[s, 0 : len(AR_PEERS[s])], s_send.at[s])

    for bt in range(4):
        total = ar_send[3, bt : bt + 1, :]
        margined, slope = margin(ar_send[3, 4 + bt : 5 + bt, :])
        losses[bt : bt + 1, :] = jnp.log(total) - margined
        scale = logit_scale / total
        rows[bt, 0:1, :] = scale
        rows[bt, 1:2, :] = (jnp.exp(margined) - total) * slope * scale

    for h in range(2):
        bt = 2 * core + h
        g_copy(h).wait()
        v = jnp.where(on_chip(bt), rows[bt, 1:2, :], 0.0)
        g = (gt[2 + h] + grecv[h].astype(f32)) * rows[bt, 0:1, :] + v * ttr[h].astype(f32)
        back = transposed(g.astype(bf16))
        for p in range(4):
            gs[p, 2 * h : 2 * h + 2] = back[:, p * 128 : (p + 1) * 128].reshape(2, 4, 4, OWN, 128)

    def rs_copy(s, p, k, order):
        axis = order[2 - s]
        to = peer(axis, k)
        if s == 0:
            src = gs.at[(p,) + tuple(to[a] if a == axis else slice(None) for a in range(3))]
            dst = rb1.at[p, k - 1]
        elif s == 1:
            left = sorted(order[:2])
            src = gs2.at[(p,) + tuple(to[a] if a == axis else slice(None) for a in left)]
            dst = rb2.at[p, k - 1]
        else:
            src = gs3.at[p]
            dst = rb3.at[p, k - 1]
        return pltpu.make_async_remote_copy(
            src_ref=src, dst_ref=dst,
            send_sem=rs_send.at[s], recv_sem=rs_recv.at[s, p],
            device_id=to, device_id_type=MESH,
        )

    def rs_start(s, p):
        def act(order):
            for k in (2, 1, 3):
                rs_copy(s, p, k, order).start()

        by_order(p, act)

    def rs_step(s):
        bufs = (rb1, rb2, rb3)[s]
        for p in range(4):
            wait_bytes(bufs.at[p], rs_recv.at[s, p])

            def act(order):
                axis = order[2 - s]
                if s == 0:
                    total = gs[(p,) + tuple(me[a] if a == axis else slice(None) for a in range(3))]
                elif s == 1:
                    total = gs2[(p,) + tuple(me[a] if a == axis else slice(None) for a in sorted(order[:2]))]
                else:
                    total = gs3[p]
                total = total.astype(f32)
                for k in (2, 1, 3):
                    total = total + bufs[p, k - 1].astype(f32)
                if s == 0:
                    gs2[p] = total.astype(bf16)
                elif s == 1:
                    gs3[p] = total.astype(bf16)
                else:
                    where = tuple(slice(None) if a == axis else me[a] for a in range(3))
                    gemb[(p, core) + where] = total.astype(bf16)
                for k in (2, 1, 3):
                    if s < 2:
                        rs_copy(s + 1, p, k, order).start()
                    else:
                        ag_copy(gemb, 1, p, 1, k, order).start()

            by_order(p, act)

    for p in range(4):
        rs_start(0, p)

    steps = {
        2: functools.partial(rs_step, 0),
        3: functools.partial(rs_step, 1),
        5: functools.partial(rs_step, 2),
        7: functools.partial(ag_next, gemb, 1, 1),
    }

    def finish_centers(i, slot):
        r = pl.ds(pl.multiple_of(i * JC, JC), JC)
        gu = gt[slot]
        cf = cen[r, :].astype(f32)
        inv = lax.rsqrt(jnp.sum(cf * cf, axis=1, keepdims=True) + epsilon)
        along = jnp.sum(gu * cf, axis=1, keepdims=True) * (inv * inv * inv)
        gc_out[r, :] = (gu * inv - cf * along).astype(bf16)

    @pl.loop(0, CLASSES // JC)
    def _(i):
        j0 = pl.multiple_of(i * JC, JC)
        r = pl.ds(j0, JC)
        gu = jnp.zeros((JC, D), f32)
        for bt in range(4):
            lab = labels[bt : bt + 1, :] - offset - j0
            hot = lab == lax.broadcasted_iota(jnp.int32, (JC, BT), 0)
            scaled = E[bt, r, :].astype(f32) * rows[bt, 0:1, :]
            gc = jnp.where(hot, rows[bt, 1:2, :], scaled).astype(bf16)
            gu = gu + plain_dot(gc, block(emb, bt))
        gt[lax.rem(i, 2)] = gu
        before = jnp.maximum(i - 1, 0)
        finish_centers(before, lax.rem(i + 1, 2))

        for at, step in steps.items():
            @pl.when(i == at)
            def _():
                step()

    finish_centers(CLASSES // JC - 1, (CLASSES // JC - 1) % 2)
    position = core * (N // 2) + chip
    line = jnp.zeros((1, BT), f32)
    for bt in range(4):
        line = jnp.where(position // 32 == bt, losses[bt : bt + 1, :], line)
    line = jnp.broadcast_to(line, (8, BT))
    for bit in (1, 2, 4, 8, 16):
        moved = pltpu.roll(line, BT - bit * OWN, 1)
        line = jnp.where(lax.rem(position // bit, 2) == 1, moved, line)
    loss_out[...] = line[:, 0:128]

    others = cols.at[pl.ds(0, N // 2 - 1)]
    pltpu.make_async_copy(others, others, a_send).wait()
    pltpu.make_async_copy(others, others, a_recv).wait()

    start = chip * 2 * F_DEV - tile_of(chip) * 128
    r = lax.broadcasted_iota(jnp.int32, (208, 384), 0)
    want = start + jnp.where(r < 104, core * F_DEV + r, (1 - core) * F_DEV + r - 104)
    pick = (lax.broadcasted_iota(jnp.int32, (208, 384), 1) == want).astype(f32).astype(bf16)
    for h in range(2):
        cols_t[h] = last_dims(pick, cols[h * 32 : (h + 1) * 32].reshape(BT, 384)).astype(bf16)

    ag_next(gemb, 1, 2)
    tangents = []
    for h in range(2):
        grad, low = (
            jnp.concatenate([buf[p, core, 2 * h : 2 * h + 2].reshape(BT, 128) for p in range(4)], axis=1).astype(f32)
            for buf in (gemb, emb)
        )
        along = jnp.sum(grad * low, axis=1, keepdims=True)
        tangents.append((grad - low * along).astype(bf16))

    def fc_rows(start):
        return sum(plain_dot(cols_t[h, start : start + 104], tangents[h]) for h in range(2))

    fc_send[...] = fc_rows(104)
    fc_copy = pltpu.make_async_remote_copy(
        src_ref=fc_send, dst_ref=fc_recv, send_sem=d_send.at[4], recv_sem=d_recv.at[4],
        device_id=peer(3, 1), device_id_type=MESH,
    )
    fc_copy.start()
    fc_own = fc_rows(0)
    fc_copy.wait()
    fc_out[...] = fc_own + fc_recv[...]

    ag_drain(emb, 0)
    ag_drain(gemb, 1)
    for s in range(3):
        wait_bytes((rb1, rb2, rb3)[s], rs_send.at[s])


def on_device(features, fc_weight, centers, labels):
    vmem = pl.BlockSpec(memory_space=pltpu.VMEM)
    anywhere = pl.BlockSpec(memory_space=pl.ANY)
    dma = pltpu.SemaphoreType.DMA
    loss, grad_fc, grad_centers = pl.pallas_call(
        kernel,
        out_shape=(
            pltpu.VMEM((8, 128), f32),
            pltpu.VMEM((104, D), f32),
            pltpu.VMEM((CLASSES, D), bf16),
        ),
        in_specs=[anywhere] * 4,
        out_specs=(vmem, vmem, vmem),
        scratch_shapes=[
            pltpu.VMEM((OWN, F), bf16),
            pltpu.VMEM((16, 128), jnp.int32),
            pltpu.VMEM((16, BT), jnp.int32),
            pltpu.VMEM((8, BT), f32),
            pltpu.VMEM((4, CLASSES, BT), bf16),
            pltpu.VMEM((CLASSES, D), bf16),
            pltpu.VMEM((CLASSES, D), bf16),
            pltpu.VMEM((D, CLASSES), bf16),
            pltpu.VMEM((4, D, BT), bf16),
            pltpu.VMEM((2, D, BT), bf16),
            pltpu.VMEM((4, 2, 4, 4, 4, OWN, 128), bf16),
            pltpu.VMEM((4, D, BT), bf16),
            pltpu.VMEM((4, 2, 4, 4, 4, OWN, 128), bf16),
            pltpu.VMEM((4, D, BT), f32),
            pltpu.VMEM((2, D, BT), bf16),
            pltpu.VMEM((2, D, BT), bf16),
            pltpu.VMEM((4, 4, 4, 4, OWN, 128), bf16),
            pltpu.VMEM((4, 3, 4, 4, OWN, 128), bf16),
            pltpu.VMEM((4, 4, 4, OWN, 128), bf16),
            pltpu.VMEM((4, 3, 4, OWN, 128), bf16),
            pltpu.VMEM((4, 4, OWN, 128), bf16),
            pltpu.VMEM((4, 3, 4, OWN, 128), bf16),
            pltpu.VMEM((N // 2, OWN, 384), bf16),
            pltpu.VMEM((2, 208, BT), bf16),
            pltpu.VMEM((104, D), f32),
            pltpu.VMEM((104, D), f32),
            pltpu.VMEM((4, 8, BT), f32),
            pltpu.VMEM((3, 7, 8, BT), f32),
            pltpu.VMEM((4, 8, BT), f32),
            dma((N_W,)),
            dma((3,)),
            dma((2, 3)),
            dma((2, 4, 3)),
            dma((5,)),
            dma((5,)),
            dma((3,)),
            dma((3, 4)),
            dma((3,)),
            dma((3,)),
            dma,
            dma,
        ],
        compiler_params=pltpu.CompilerParams(
            collective_id=0, has_side_effects=True, vmem_limit_bytes=58_000_000
        ),
    )(features, fc_weight, centers, labels.reshape(16, 128))
    return (loss[0, :OWN], grad_centers, grad_fc[:F_DEV])


def solution(mesh):
    torus = Mesh(mesh.devices.reshape(4, 4, 4, 2), CLS)
    placed = (P(CLS, None), P(), P(CLS, None), P())
    return jax.shard_map(
        on_device,
        mesh=torus,
        in_specs=placed,
        out_specs=(P(CLS), P(CLS, None), P(CLS, None)),
        check_vma=False,
    )
```
